256 devices in a mesh: fsdp: 16 (over z, core), cols: 16 (over y, x).
Axes of the slice: x: 4, y: 4, z: 8, core: 2. Of those that a mesh axis runs over, the one named last changes fastest.
Arguments:
- one_query: float32 [4096, 4096], P('fsdp', 'cols'), may hold values from -0.125 to 0.125
- other_query: float32 [4096, 4096], P('fsdp', 'cols'), may hold values from -0.09375 to 0.09375
- one_key: float32 [4096, 4096], P('fsdp', 'cols'), may hold values from -0.125 to 0.125
- other_key: float32 [4096, 4096], P('fsdp', 'cols'), may hold values from -0.09375 to 0.09375
- one_value: float32 [4096, 4096], P('fsdp', 'cols'), may hold values from -0.125 to 0.125
- other_value: float32 [4096, 4096], P('fsdp', 'cols'), may hold values from -0.09375 to 0.09375
- mix_share: float32 [4096], P('fsdp'), may hold values from 0.2 to 0.8
- norm_train: float32 [4096], P(('fsdp', 'cols')), may hold values from 0.25 to 1.75
- norm_step: float32 [4096], P(('fsdp', 'cols')), may hold values from -0.3 to 0.3
Outputs:
- final_query: bfloat16 [4096, 4096], P(None, 'cols')
- final_key: bfloat16 [4096, 4096], P(None, 'cols')
- final_value: bfloat16 [4096, 4096], P(None, 'cols')
- scale_query: float32 [4096], P('cols')
- scale_key: float32 [4096], P('cols')
- scale_value: float32 [4096], P('cols')
- serve_norm: bfloat16 [4096], replicated
The draws below stay inside these ranges and needn't reach their ends.
All inputs are finite; a program needn't handle non-finite values.
Results may differ from the reference program's by a relative error of at most 0.0004.
Values may be sent and summed in bfloat16 or wider, within the bound.
A program may use at most 64 MiB of HBM per device.

```python
import jax
import jax.numpy as jnp
from jax import lax

D_MODEL = 4096
Q_DIM = 4096
KV_DIM = 4096


def with_spikes(values, stream_key, source, target, shards_of, factor):
    owner, partner = [(jnp.arange(values.shape[position]) // (values.shape[position] // shards_of)).reshape([-1 if axis == position else 1 for axis in range(values.ndim)]) for position in (source, target)]
    chosen = jax.random.permutation(stream_key, shards_of)[partner]
    strong = (owner == chosen) | (owner == (partner + shards_of // 2) % shards_of)
    return jnp.where(strong, factor * values, values)


def level_of(rng, extent, split, low, top_value):
    loudness = 1.0
    for position, parts in split:
        steps = jax.random.uniform(jax.random.fold_in(jax.random.fold_in(rng, 6), position), (parts,), jnp.float32, low / len(split), top_value / len(split))
        loudness = loudness * jnp.repeat(jnp.exp(steps), extent[position] // parts).reshape((-1,) + (1,) * (len(extent) - 1 - position))
    return loudness


def noise(stream_key, dims, deviation, limit, shards=(), held_as=jnp.bfloat16):
    factor_of = level_of(stream_key, dims, shards, -0.22, 0.18) if shards else 1.0
    drawn = jax.random.normal(stream_key, dims, jnp.float32) * deviation * factor_of
    return jnp.minimum(jnp.maximum(drawn, -limit), limit).astype(held_as)


def gaussian_with(stream_key, dims, scale, most, cuts, heavy, dtype=jnp.bfloat16):
    values = scale * jax.random.normal(stream_key, dims, jnp.float32)
    if cuts:
        values = values * level_of(stream_key, dims, cuts, -0.22, 0.18)
    return jnp.clip(with_spikes(values, jax.random.fold_in(stream_key, 3), *heavy), -most, most).astype(dtype)


def setup_inputs(seed: int = 0) -> dict:
    key_list = jax.random.split(jax.random.key(seed), 10)
    one_query = gaussian_with(key_list[0], (D_MODEL, Q_DIM), D_MODEL ** -0.5, 0.125, ((0, 16), (1, 16)), (0, 1, 16, 2.0), jnp.float32)
    other_query = noise(key_list[1], (D_MODEL, Q_DIM), D_MODEL ** -0.5, 0.09375, ((0, 16), (1, 16)), jnp.float32)
    one_key = gaussian_with(key_list[2], (D_MODEL, KV_DIM), D_MODEL ** -0.5, 0.125, ((0, 16), (1, 16)), (0, 1, 16, 2.0), jnp.float32)
    other_key = noise(key_list[3], (D_MODEL, KV_DIM), D_MODEL ** -0.5, 0.09375, ((0, 16), (1, 16)), jnp.float32)
    one_value = gaussian_with(key_list[4], (D_MODEL, KV_DIM), D_MODEL ** -0.5, 0.125, ((0, 16), (1, 16)), (0, 1, 16, 2.0), jnp.float32)
    other_value = noise(key_list[5], (D_MODEL, KV_DIM), D_MODEL ** -0.5, 0.09375, ((0, 16), (1, 16)), jnp.float32)
    mix_share = jnp.clip(0.2 + 0.6 * jax.random.uniform(key_list[6], (D_MODEL,), jnp.float32) ** level_of(key_list[6], (D_MODEL,), ((0, 16),), -0.2, 0.2), 0.2, 0.8)
    norm_train = jnp.clip(1.0 + 0.15 * jax.random.normal(key_list[7], (D_MODEL,), jnp.float32), 0.25, 1.75)
    norm_step = jnp.clip(jax.random.uniform(key_list[8], (D_MODEL,), jnp.float32, -0.3, 0.3) * level_of(key_list[8], (D_MODEL,), ((0, 256),), -0.4, 0.0), -0.3, 0.3)
    return dict(one_query=one_query, other_query=other_query, one_key=one_key, other_key=other_key, one_value=one_value, other_value=other_value, mix_share=mix_share, norm_train=norm_train, norm_step=norm_step)


def reference(one_query, other_query, one_key, other_key, one_value, other_value, mix_share, norm_train, norm_step):
    result_query = mix_share[:, None] * one_query + (1.0 - mix_share[:, None]) * other_query
    result_key = mix_share[:, None] * one_key + (1.0 - mix_share[:, None]) * other_key
    result_value = mix_share[:, None] * one_value + (1.0 - mix_share[:, None]) * other_value
    scale_query = jnp.sqrt(lax.optimization_barrier(jnp.sum(result_query * result_query, axis=0)))
    final_query = (result_query / scale_query).astype(jnp.bfloat16)
    scale_key = jnp.sqrt(lax.optimization_barrier(jnp.sum(result_key * result_key, axis=0)))
    final_key = (result_key / scale_key).astype(jnp.bfloat16)
    scale_value = jnp.sqrt(lax.optimization_barrier(jnp.sum(result_value * result_value, axis=0)))
    final_value = (result_value / scale_value).astype(jnp.bfloat16)
    serve_norm = (norm_train + norm_step).astype(jnp.bfloat16)
    return (final_query, final_key, final_value, scale_query, scale_key, scale_value, serve_norm)
```

```python
import functools

import jax
import jax.numpy as jnp
from jax import lax
from jax.experimental import pallas as pl
from jax.experimental.pallas import tpu as pltpu
from jax.sharding import Mesh
from jax.sharding import PartitionSpec as P

FSDP = ("fsdp_0", "fsdp_1")
FSDP_COLS = ("fsdp_0", "fsdp_1", "cols_0", "cols_1")
COLS = ("cols_0", "cols_1")
MESH = pl.DeviceIdType.MESH

Z = 8
CORES = 2
SHARDS = Z * CORES
PLANE_Y = 4
PLANE_X = 4
PLANE = PLANE_Y * PLANE_X
ROWS = 256
HALF = 128
LANES = 128
PIECE = 16
NEAR = [(d, a, h) for d in (1, 2, 3) for a in range(3) for h in range(2)]
STREAM = (
    NEAR + [(4, a, 0) for a in range(3)],
    NEAR + [(4, a, 1) for a in range(3)],
)
STEPS = len(STREAM[0])


def kernel(
    oq, tq, ok, tk, ov, tv, share, train, step,
    out_q, out_k, out_v, scale_q, scale_k, scale_v, norm,
    ins, share_v, norm_in, mixed, msg, sums, plane_out, plane_in, norm_f32,
    in_sem, sum_send, sum_recv, plane_send, plane_recv,
    ici_send, ici_recv, own_send, own_recv, d2d_send, d2d_recv,
):
    z, c = lax.axis_index("fsdp_0"), lax.axis_index("fsdp_1")
    col = lax.axis_index("cols_0") * PLANE_X + lax.axis_index("cols_1")
    me = z * CORES + c
    outs = (out_q, out_k, out_v)

    def fsdp_peers():
        for dz in (4, 5, 3, 6, 2, 7, 1, 0):
            for dc in (0, 1):
                if dz or dc:
                    pz, pc = lax.rem(z + dz, Z), lax.rem(c + dc, CORES)
                    yield {"fsdp_0": pz, "fsdp_1": pc}, pz * CORES + pc

    def plane_peers():
        for k in range(1, PLANE):
            p = lax.rem(col + k, PLANE)
            yield {"cols_0": p // PLANE_X, "cols_1": lax.rem(p, PLANE_X)}, p

    barrier = pltpu.get_barrier_semaphore()
    for device, _ in list(fsdp_peers()) + list(plane_peers()):
        pl.semaphore_signal(barrier, inc=1, device_id=device, device_id_type=MESH)

    loads = [pltpu.make_async_copy(share, share_v, in_sem.at[6])]
    loads += [
        pltpu.make_async_copy(src, ins.at[i], in_sem.at[i])
        for i, src in enumerate((oq, tq, ok, tk, ov, tv))
    ]
    loads += [
        pltpu.make_async_copy(train, norm_in.at[0], in_sem.at[7]),
        pltpu.make_async_copy(step, norm_in.at[1], in_sem.at[8]),
    ]
    for load in loads:
        load.start()

    msg[...] = jnp.zeros_like(msg)
    loads[0].wait()
    shares = [
        jnp.broadcast_to(share_v[:, r * HALF : (r + 1) * HALF], (LANES, HALF)).T for r in range(2)
    ]
    for a in range(3):
        loads[1 + 2 * a].wait()
        loads[2 + 2 * a].wait()
        for j in range(2):
            lanes = pl.ds(j * LANES, LANES)
            total = jnp.zeros((1, LANES), jnp.float32)
            for r in range(2):
                rows = pl.ds(r * HALF, HALF)
                value = shares[r] * ins[2 * a, rows, lanes] + (1.0 - shares[r]) * ins[2 * a + 1, rows, lanes]
                mixed[a, rows, lanes] = value
                total = total + jnp.sum(value * value, axis=0, keepdims=True)
            msg[pl.ds(2 * a + j, 1), :] = total
    loads[7].wait()
    loads[8].wait()
    piece = jnp.concatenate(
        [norm_in[0] + norm_in[1], jnp.zeros((1, LANES - PIECE), jnp.float32)], axis=1
    )
    piece = pltpu.roll(jnp.broadcast_to(piece, (8, LANES)), lax.rem(col, 8) * PIECE, 1)
    msg[pl.ds(6, 1), :] = piece[:1]

    pl.semaphore_wait(barrier, SHARDS - 1 + PLANE - 1)

    exchanges = []
    for device, p in fsdp_peers():
        copy = pltpu.make_async_remote_copy(
            src_ref=msg, dst_ref=sums.at[me], send_sem=sum_send.at[p], recv_sem=sum_recv.at[me],
            device_id=device, device_id_type=MESH,
        )
        copy.start()
        exchanges.append(copy)
    sums[pl.ds(me, 1)] = msg[...][None]
    arrivals = []
    for device, p in fsdp_peers():
        arrivals.append(pltpu.make_async_remote_copy(
            src_ref=msg, dst_ref=sums.at[p], send_sem=sum_send.at[p], recv_sem=sum_recv.at[p],
            device_id=device, device_id_type=MESH,
        ))
    for copy in arrivals:
        copy.wait_recv()

    total = sums[0]
    for s in range(1, SHARDS):
        total = total + sums[s]
    scale = jnp.sqrt(total)
    inverse = 1.0 / scale
    own = pl.multiple_of(me * ROWS, ROWS)
    for a, out in enumerate(outs):
        for r in range(2):
            for j in range(2):
                lanes = pl.ds(j * LANES, LANES)
                value = mixed[a, pl.ds(r * HALF, HALF), lanes] * inverse[2 * a + j : 2 * a + j + 1]
                out[pl.ds(pl.multiple_of(own + r * HALF, HALF), HALF), lanes] = value.astype(jnp.bfloat16)

    def chunk(shard, a, h):
        return outs[a].at[pl.ds(pl.multiple_of(shard * ROWS + h * HALF, HALF), HALF)]

    def along(way, i):
        d, a, h = STREAM[way][i]
        source = lax.rem(z + (Z - d if way == 0 else d), Z)
        return source * CORES + c, a, h

    def hop(way, i, shard, a, h):
        ref = chunk(shard, a, h)
        target = lax.rem(z + (1 if way == 0 else Z - 1), Z)
        return pltpu.make_async_remote_copy(
            src_ref=ref, dst_ref=ref, send_sem=ici_send.at[way, i], recv_sem=ici_recv.at[way, i],
            device_id={"fsdp_0": target}, device_id_type=MESH,
        )

    def across(send, recv, shard, a, h):
        ref = chunk(shard, a, h)
        return pltpu.make_async_remote_copy(
            src_ref=ref, dst_ref=ref, send_sem=send, recv_sem=recv,
            device_id={"fsdp_1": 1 - c}, device_id_type=MESH,
        )

    sent = list(exchanges)
    for a in range(3):
        for h in range(2):
            for way in range(2):
                copy = hop(way, 2 * a + h, me, a, h)
                copy.start()
                sent.append(copy)
    for a in range(3):
        for h in range(2):
            copy = across(own_send.at[2 * a + h], own_recv.at[2 * a + h], me, a, h)
            copy.start()
            sent.append(copy)

    for a, ref in enumerate((scale_q, scale_k, scale_v)):
        for j in range(2):
            ref[:, pl.ds(j * LANES, LANES)] = scale[2 * a + j : 2 * a + j + 1]

    for s in range(SHARDS):
        plane_out[pl.ds(s, 1), :] = sums[s, 6:7, :]
    for device, p in plane_peers():
        copy = pltpu.make_async_remote_copy(
            src_ref=plane_out, dst_ref=plane_in.at[col], send_sem=plane_send.at[p], recv_sem=plane_recv.at[col],
            device_id=device, device_id_type=MESH,
        )
        copy.start()
        sent.append(copy)
    plane_in[pl.ds(col, 1)] = plane_out[...][None]

    for i in range(STEPS):
        for way in range(2):
            d, a, h = STREAM[way][i]
            shard, _, _ = along(way, i)
            hop(way, i, shard, a, h).wait_recv()
            if (d + 1, a, h) in STREAM[way]:
                copy = hop(way, STREAM[way].index((d + 1, a, h)), shard, a, h)
                copy.start()
                sent.append(copy)
            copy = across(d2d_send.at[way, i], d2d_recv.at[way, i], shard, a, h)
            copy.start()
            sent.append(copy)

    for device, p in plane_peers():
        pltpu.make_async_remote_copy(
            src_ref=plane_out, dst_ref=plane_in.at[p], send_sem=plane_send.at[p], recv_sem=plane_recv.at[p],
            device_id=device, device_id_type=MESH,
        ).wait_recv()
    for side in range(2):
        gathered = plane_in[8 * side]
        for k in range(1, 8):
            gathered = gathered + plane_in[8 * side + k]
        norm_f32[pl.ds(side, SHARDS, stride=2), :] = gathered
    norm[...] = norm_f32[...].astype(jnp.bfloat16)

    partner = z * CORES + 1 - c
    for a in range(3):
        for h in range(2):
            across(own_send.at[2 * a + h], own_recv.at[2 * a + h], partner, a, h).wait_recv()
    for i in range(STEPS):
        for way in range(2):
            shard, a, h = along(way, i)
            across(d2d_send.at[way, i], d2d_recv.at[way, i], shard + 1 - 2 * c, a, h).wait_recv()
    for copy in sent:
        copy.wait_send()


def per_device(oq, tq, ok, tk, ov, tv, share, train, step):
    f32, bf16 = jnp.float32, jnp.bfloat16
    whole = jax.ShapeDtypeStruct((SHARDS * ROWS, 2 * LANES), bf16)
    scale = jax.ShapeDtypeStruct((1, 2 * LANES), f32)
    vmem = pl.BlockSpec(memory_space=pltpu.VMEM)
    dma = pltpu.SemaphoreType.DMA
    outs = pl.pallas_call(
        kernel,
        name="mix_and_gather",
        out_shape=(whole, whole, whole, scale, scale, scale, jax.ShapeDtypeStruct((32, LANES), bf16)),
        in_specs=[pl.BlockSpec(memory_space=pl.ANY)] * 9,
        out_specs=(vmem,) * 7,
        scratch_shapes=[
            pltpu.VMEM((6, ROWS, 2 * LANES), f32),
            pltpu.VMEM((1, ROWS), f32),
            pltpu.VMEM((2, 1, PIECE), f32),
            pltpu.VMEM((3, ROWS, 2 * LANES), f32),
            pltpu.VMEM((8, LANES), f32),
            pltpu.VMEM((SHARDS, 8, LANES), f32),
            pltpu.VMEM((SHARDS, LANES), f32),
            pltpu.VMEM((PLANE, SHARDS, LANES), f32),
            pltpu.VMEM((32, LANES), f32),
            dma((9,)),
            dma((SHARDS,)),
            dma((SHARDS,)),
            dma((PLANE,)),
            dma((PLANE,)),
            dma((2, STEPS)),
            dma((2, STEPS)),
            dma((6,)),
            dma((6,)),
            dma((2, STEPS)),
            dma((2, STEPS)),
        ],
        compiler_params=pltpu.CompilerParams(collective_id=0, has_side_effects=True),
    )(oq, tq, ok, tk, ov, tv, share.reshape(1, -1), train.reshape(1, -1), step.reshape(1, -1))
    q, k, v, scale_q, scale_k, scale_v, norm = outs
    return q, k, v, scale_q.reshape(-1), scale_k.reshape(-1), scale_v.reshape(-1), norm.reshape(-1)


def solution(mesh):
    split = Mesh(mesh.devices.reshape(Z, CORES, PLANE_Y, PLANE_X), FSDP_COLS)
    block = P(FSDP, COLS)
    return jax.shard_map(
        per_device,
        mesh=split,
        in_specs=(block,) * 6 + (P(FSDP), P(FSDP_COLS), P(FSDP_COLS)),
        out_specs=(P(None, COLS),) * 3 + (P(COLS),) * 3 + (P(),),
        check_vma=False,
    )
```

```python
import functools

import jax
import jax.numpy as jnp
from jax import lax
from jax.experimental import pallas as pl
from jax.experimental.pallas import tpu as pltpu
from jax.sharding import Mesh
from jax.sharding import PartitionSpec as P

FSDP = ("fsdp_0", "fsdp_1")
FSDP_COLS = ("fsdp_0", "fsdp_1", "cols_0", "cols_1")
COLS = ("cols_0", "cols_1")
MESH = pl.DeviceIdType.MESH

Z = 8
CORES = 2
SHARDS = Z * CORES
PLANE_Y = 4
PLANE_X = 4
PLANE = PLANE_Y * PLANE_X
ROWS = 256
HALF = 128
LANES = 128
PIECE = 16
NEAR = [(d, a, h) for d in (1, 2, 3) for a in range(3) for h in range(2)]
STREAM = (
    NEAR + [(4, a, 0) for a in range(3)],
    NEAR + [(4, a, 1) for a in range(3)],
)
STEPS = len(STREAM[0])


def kernel(
    oq, tq, ok, tk, ov, tv, share, train, step,
    out_q, out_k, out_v, scale_q, scale_k, scale_v, norm,
    ins, share_v, norm_in, mixed, msg, sums, plane_out, plane_in, norm_f32,
    in_sem, sum_send, sum_recv, plane_send, plane_recv,
    ici_send, ici_recv, own_send, own_recv, d2d_send, d2d_recv,
):
    z, c = lax.axis_index("fsdp_0"), lax.axis_index("fsdp_1")
    col = lax.axis_index("cols_0") * PLANE_X + lax.axis_index("cols_1")
    me = z * CORES + c
    outs = (out_q, out_k, out_v)

    def fsdp_peers():
        for dz in (4, 5, 3, 6, 2, 7, 1, 0):
            for dc in (0, 1):
                if dz or dc:
                    pz, pc = lax.rem(z + dz, Z), lax.rem(c + dc, CORES)
                    yield {"fsdp_0": pz, "fsdp_1": pc}, pz * CORES + pc

    def plane_peers():
        for k in range(1, PLANE):
            p = lax.rem(col + k, PLANE)
            yield {"cols_0": p // PLANE_X, "cols_1": lax.rem(p, PLANE_X)}, p

    barrier = pltpu.get_barrier_semaphore()
    for device, _ in list(fsdp_peers()) + list(plane_peers()):
        pl.semaphore_signal(barrier, inc=1, device_id=device, device_id_type=MESH)

    loads = [pltpu.make_async_copy(share, share_v, in_sem.at[6])]
    loads += [
        pltpu.make_async_copy(src, ins.at[i], in_sem.at[i])
        for i, src in enumerate((oq, tq, ok, tk, ov, tv))
    ]
    loads += [
        pltpu.make_async_copy(train, norm_in.at[0], in_sem.at[7]),
        pltpu.make_async_copy(step, norm_in.at[1], in_sem.at[8]),
    ]
    for load in loads:
        load.start()

    msg[...] = jnp.zeros_like(msg)
    loads[0].wait()
    shares = [
        jnp.broadcast_to(share_v[:, r * HALF : (r + 1) * HALF], (LANES, HALF)).T for r in range(2)
    ]
    for a in range(3):
        loads[1 + 2 * a].wait()
        loads[2 + 2 * a].wait()
        for j in range(2):
            lanes = pl.ds(j * LANES, LANES)
            total = jnp.zeros((1, LANES), jnp.float32)
            for r in range(2):
                rows = pl.ds(r * HALF, HALF)
                value = shares[r] * ins[2 * a, rows, lanes] + (1.0 - shares[r]) * ins[2 * a + 1, rows, lanes]
                mixed[a, rows, lanes] = value
                total = total + jnp.sum(value * value, axis=0, keepdims=True)
            msg[pl.ds(2 * a + j, 1), :] = total
    loads[7].wait()
    loads[8].wait()
    piece = jnp.concatenate(
        [norm_in[0] + norm_in[1], jnp.zeros((1, LANES - PIECE), jnp.float32)], axis=1
    )
    piece = pltpu.roll(jnp.broadcast_to(piece, (8, LANES)), lax.rem(col, 8) * PIECE, 1)
    msg[pl.ds(6, 1), :] = piece[:1]

    pl.semaphore_wait(barrier, SHARDS - 1 + PLANE - 1)

    exchanges = []
    for device, p in fsdp_peers():
        copy = pltpu.make_async_remote_copy(
            src_ref=msg, dst_ref=sums.at[me], send_sem=sum_send.at[p], recv_sem=sum_recv.at[me],
            device_id=device, device_id_type=MESH,
        )
        copy.start()
        exchanges.append(copy)
    sums[pl.ds(me, 1)] = msg[...][None]
    arrivals = []
    for device, p in fsdp_peers():
        arrivals.append(pltpu.make_async_remote_copy(
            src_ref=msg, dst_ref=sums.at[p], send_sem=sum_send.at[p], recv_sem=sum_recv.at[p],
            device_id=device, device_id_type=MESH,
        ))
    for copy in arrivals:
        copy.wait_recv()

    total = sums[0]
    for s in range(1, SHARDS):
        total = total + sums[s]
    scale = jnp.sqrt(total)
    inverse = 1.0 / scale
    own = pl.multiple_of(me * ROWS, ROWS)
    for a, out in enumerate(outs):
        for r in range(2):
            for j in range(2):
                lanes = pl.ds(j * LANES, LANES)
                value = mixed[a, pl.ds(r * HALF, HALF), lanes] * inverse[2 * a + j : 2 * a + j + 1]
                out[pl.ds(pl.multiple_of(own + r * HALF, HALF), HALF), lanes] = value.astype(jnp.bfloat16)

    def chunk(shard, a, h):
        return outs[a].at[pl.ds(pl.multiple_of(shard * ROWS + h * HALF, HALF), HALF)]

    def along(way, i):
        d, a, h = STREAM[way][i]
        source = lax.rem(z + (Z - d if way == 0 else d), Z)
        return source * CORES + c, a, h

    def hop(way, i, shard, a, h):
        ref = chunk(shard, a, h)
        target = lax.rem(z + (1 if way == 0 else Z - 1), Z)
        return pltpu.make_async_remote_copy(
            src_ref=ref, dst_ref=ref, send_sem=ici_send.at[way, i], recv_sem=ici_recv.at[way, i],
            device_id={"fsdp_0": target}, device_id_type=MESH,
        )

    def across(send, recv, shard, a, h):
        ref = chunk(shard, a, h)
        return pltpu.make_async_remote_copy(
            src_ref=ref, dst_ref=ref, send_sem=send, recv_sem=recv,
            device_id={"fsdp_1": 1 - c}, device_id_type=MESH,
        )

    sent = list(exchanges)
    for a in range(3):
        for h in range(2):
            for way in range(2):
                copy = hop(way, 2 * a + h, me, a, h)
                copy.start()
                sent.append(copy)
    for a in range(3):
        for h in range(2):
            copy = across(own_send.at[2 * a + h], own_recv.at[2 * a + h], me, a, h)
            copy.start()
            sent.append(copy)

    for a, ref in enumerate((scale_q, scale_k, scale_v)):
        for j in range(2):
            ref[:, pl.ds(j * LANES, LANES)] = scale[2 * a + j : 2 * a + j + 1]

    for s in range(SHARDS):
        plane_out[pl.ds(s, 1), :] = sums[s, 6:7, :]
    for device, p in plane_peers():
        copy = pltpu.make_async_remote_copy(
            src_ref=plane_out, dst_ref=plane_in.at[col], send_sem=plane_send.at[p], recv_sem=plane_recv.at[col],
            device_id=device, device_id_type=MESH,
        )
        copy.start()
        sent.append(copy)
    plane_in[pl.ds(col, 1)] = plane_out[...][None]

    for i in range(STEPS):
        for way in range(2):
            d, a, h = STREAM[way][i]
            shard, _, _ = along(way, i)
            hop(way, i, shard, a, h).wait_recv()
            if (d + 1, a, h) in STREAM[way]:
                copy = hop(way, STREAM[way].index((d + 1, a, h)), shard, a, h)
                copy.start()
                sent.append(copy)
            copy = across(d2d_send.at[way, i], d2d_recv.at[way, i], shard, a, h)
            copy.start()
            sent.append(copy)

    for device, p in plane_peers():
        pltpu.make_async_remote_copy(
            src_ref=plane_out, dst_ref=plane_in.at[p], send_sem=plane_send.at[p], recv_sem=plane_recv.at[p],
            device_id=device, device_id_type=MESH,
        ).wait_recv()
    for side in range(2):
        gathered = plane_in[8 * side]
        for k in range(1, 8):
            gathered = gathered + plane_in[8 * side + k]
        norm_f32[pl.ds(side, SHARDS, stride=2), :] = gathered
    norm[...] = norm_f32[...].astype(jnp.bfloat16)

    partner = z * CORES + 1 - c
    for a in range(3):
        for h in range(2):
            across(own_send.at[2 * a + h], own_recv.at[2 * a + h], partner, a, h).wait_recv()
    for i in range(STEPS):
        for way in range(2):
            shard, a, h = along(way, i)
            across(d2d_send.at[way, i], d2d_recv.at[way, i], shard + 1 - 2 * c, a, h).wait_recv()
    for copy in sent:
        copy.wait_send()


PARTS = 4


def store_kernel(*refs):
    ins, outs, sem = refs[:7], refs[7:14], refs[14]
    copies = []
    for i, (src, dst) in enumerate(zip(ins, outs)):
        parts = PARTS if i < 3 else 1
        rows = src.shape[0] // parts
        for p in range(parts):
            window = pl.ds(p * rows, rows)
            copies.append(pltpu.make_async_copy(src.at[window], dst.at[window], sem.at[len(copies)]))
    for copy in copies:
        copy.start()
    for copy in copies:
        copy.wait()


def store(arrays):
    return pl.pallas_call(
        store_kernel,
        name="store",
        out_shape=tuple(jax.ShapeDtypeStruct(a.shape, a.dtype) for a in arrays),
        in_specs=[pl.BlockSpec(memory_space=pltpu.VMEM)] * 7,
        out_specs=(pl.BlockSpec(memory_space=pltpu.HBM),) * 7,
        scratch_shapes=[pltpu.SemaphoreType.DMA((3 * PARTS + 4,))],
        compiler_params=pltpu.CompilerParams(vmem_limit_bytes=16 * 2**20),
    )(*arrays)


def per_device(oq, tq, ok, tk, ov, tv, share, train, step):
    f32, bf16 = jnp.float32, jnp.bfloat16
    whole = jax.ShapeDtypeStruct((SHARDS * ROWS, 2 * LANES), bf16)
    scale = jax.ShapeDtypeStruct((1, 2 * LANES), f32)
    vmem = pl.BlockSpec(memory_space=pltpu.VMEM)
    dma = pltpu.SemaphoreType.DMA
    outs = pl.pallas_call(
        kernel,
        name="mix_and_gather",
        out_shape=(whole, whole, whole, scale, scale, scale, jax.ShapeDtypeStruct((32, LANES), bf16)),
        in_specs=[pl.BlockSpec(memory_space=pltpu.HBM)] * 9,
        out_specs=(vmem,) * 7,
        scratch_shapes=[
            pltpu.VMEM((6, ROWS, 2 * LANES), f32),
            pltpu.VMEM((1, ROWS), f32),
            pltpu.VMEM((2, 1, PIECE), f32),
            pltpu.VMEM((3, ROWS, 2 * LANES), f32),
            pltpu.VMEM((8, LANES), f32),
            pltpu.VMEM((SHARDS, 8, LANES), f32),
            pltpu.VMEM((SHARDS, LANES), f32),
            pltpu.VMEM((PLANE, SHARDS, LANES), f32),
            pltpu.VMEM((32, LANES), f32),
            dma((9,)),
            dma((SHARDS,)),
            dma((SHARDS,)),
            dma((PLANE,)),
            dma((PLANE,)),
            dma((2, STEPS)),
            dma((2, STEPS)),
            dma((6,)),
            dma((6,)),
            dma((2, STEPS)),
            dma((2, STEPS)),
        ],
        compiler_params=pltpu.CompilerParams(collective_id=0, has_side_effects=True, vmem_limit_bytes=24 * 2**20),
    )(*(pltpu.with_memory_space_constraint(a, pltpu.HBM) for a in (
        oq, tq, ok, tk, ov, tv, share.reshape(1, -1), train.reshape(1, -1), step.reshape(1, -1)
    )))
    q, k, v, scale_q, scale_k, scale_v, norm = store(outs)
    return q, k, v, scale_q.reshape(-1), scale_k.reshape(-1), scale_v.reshape(-1), norm.reshape(-1)


def solution(mesh):
    split = Mesh(mesh.devices.reshape(Z, CORES, PLANE_Y, PLANE_X), FSDP_COLS)
    block = P(FSDP, COLS)
    return jax.shard_map(
        per_device,
        mesh=split,
        in_specs=(block,) * 6 + (P(FSDP), P(FSDP_COLS), P(FSDP_COLS)),
        out_specs=(P(None, COLS),) * 3 + (P(COLS),) * 3 + (P(),),
        check_vma=False,
    )
```

```python
import functools

import jax
import jax.numpy as jnp
from jax import lax
from jax.experimental import pallas as pl
from jax.experimental.pallas import tpu as pltpu
from jax.sharding import Mesh
from jax.sharding import PartitionSpec as P

FSDP = ("fsdp_0", "fsdp_1")
FSDP_COLS = ("fsdp_0", "fsdp_1", "cols_0", "cols_1")
COLS = ("cols_0", "cols_1")
MESH = pl.DeviceIdType.MESH

Z = 8
CORES = 2
SHARDS = Z * CORES
PLANE_Y = 4
PLANE_X = 4
PLANE = PLANE_Y * PLANE_X
ROWS = 256
HALF = 128
LANES = 128
PIECE = 16
NEAR = [(d, a, h) for d in (1, 2, 3) for a in range(3) for h in range(2)]
STREAM = (
    NEAR + [(4, a, 0) for a in range(3)],
    NEAR + [(4, a, 1) for a in range(3)],
)
STEPS = len(STREAM[0])
EARLY = [(0, 0), (0, 1)]
ANSWER = 8


def kernel(
    oq, tq, ok, tk, ov, tv, share, train, step,
    out_q, out_k, out_v, scale_q, scale_k, scale_v, norm,
    ins, share_v, norm_in, mixed, landed, msg, sums, plane_out, plane_in, norm_f32,
    in_sem, sum_send, sum_recv, plane_send, plane_recv, answer_send, answer_recv,
    ici_send, ici_recv, own_send, own_recv, d2d_send, d2d_recv,
):
    z, c = lax.axis_index("fsdp_0"), lax.axis_index("fsdp_1")
    col = lax.axis_index("cols_0") * PLANE_X + lax.axis_index("cols_1")
    me = z * CORES + c
    outs = (out_q, out_k, out_v)

    def fsdp_peers():
        for dz in (4, 5, 3, 6, 2, 7, 1, 0):
            for dc in (0, 1):
                if dz or dc:
                    pz, pc = lax.rem(z + dz, Z), lax.rem(c + dc, CORES)
                    yield {"fsdp_0": pz, "fsdp_1": pc}, pz * CORES + pc

    def plane_peers():
        for p in range(1, PLANE):
            yield {"cols_0": p // PLANE_X, "cols_1": p % PLANE_X}, p

    barrier = pltpu.get_barrier_semaphore()
    for device, _ in fsdp_peers():
        pl.semaphore_signal(barrier, inc=1, device_id=device, device_id_type=MESH)

    @pl.when(col == 0)
    def _():
        for device, _ in plane_peers():
            pl.semaphore_signal(barrier, inc=1, device_id=device, device_id_type=MESH)

    def chunk(shard, a, h):
        return outs[a].at[pl.ds(pl.multiple_of(shard * ROWS + h * HALF, HALF), HALF)]

    def along(way, i):
        d, a, h = STREAM[way][i]
        source = lax.rem(z + (Z - d if way == 0 else d), Z)
        return source * CORES + c, a, h

    def hop(way, i, shard, a, h):
        ref = chunk(shard, a, h)
        target = lax.rem(z + (1 if way == 0 else Z - 1), Z)
        return pltpu.make_async_remote_copy(
            src_ref=ref, dst_ref=ref, send_sem=ici_send.at[way, i], recv_sem=ici_recv.at[way, i],
            device_id={"fsdp_0": target}, device_id_type=MESH,
        )

    def early(way, e):
        a, h = EARLY[e]
        i = STREAM[way].index((1, a, h))
        target = lax.rem(z + (1 if way == 0 else Z - 1), Z)
        return pltpu.make_async_remote_copy(
            src_ref=mixed.at[a, pl.ds(h * HALF, HALF)], dst_ref=landed.at[way, e],
            send_sem=ici_send.at[way, i], recv_sem=ici_recv.at[way, i],
            device_id={"fsdp_0": target}, device_id_type=MESH,
        )

    def across(send, recv, shard, a, h):
        ref = chunk(shard, a, h)
        return pltpu.make_async_remote_copy(
            src_ref=ref, dst_ref=ref, send_sem=send, recv_sem=recv,
            device_id={"fsdp_1": 1 - c}, device_id_type=MESH,
        )

    loads = [pltpu.make_async_copy(share, share_v, in_sem.at[6])]
    loads += [
        pltpu.make_async_copy(src, ins.at[i], in_sem.at[i])
        for i, src in enumerate((oq, tq, ok, tk, ov, tv))
    ]
    loads += [
        pltpu.make_async_copy(train, norm_in.at[0], in_sem.at[7]),
        pltpu.make_async_copy(step, norm_in.at[1], in_sem.at[8]),
    ]
    for load in loads:
        load.start()

    msg[...] = jnp.zeros_like(msg)
    loads[0].wait()
    shares = [
        jnp.broadcast_to(share_v[:, r * HALF : (r + 1) * HALF], (LANES, HALF)).T for r in range(2)
    ]
    for a in range(3):
        loads[1 + 2 * a].wait()
        loads[2 + 2 * a].wait()
        for j in range(2):
            lanes = pl.ds(j * LANES, LANES)
            total = jnp.zeros((1, LANES), jnp.float32)
            for r in range(2):
                rows = pl.ds(r * HALF, HALF)
                value = shares[r] * ins[2 * a, rows, lanes] + (1.0 - shares[r]) * ins[2 * a + 1, rows, lanes]
                mixed[a, rows, lanes] = value
                total = total + jnp.sum(value * value, axis=0, keepdims=True)
            msg[pl.ds(2 * a + j, 1), :] = total
    loads[7].wait()
    loads[8].wait()
    piece = jnp.concatenate(
        [norm_in[0] + norm_in[1], jnp.zeros((1, LANES - PIECE), jnp.float32)], axis=1
    )
    piece = pltpu.roll(jnp.broadcast_to(piece, (8, LANES)), lax.rem(col, 8) * PIECE, 1)
    msg[pl.ds(6, 1), :] = piece[:1]

    pl.semaphore_wait(barrier, SHARDS - 1 + (col + PLANE - 1) // PLANE)

    exchanges = []
    for device, p in fsdp_peers():
        copy = pltpu.make_async_remote_copy(
            src_ref=msg, dst_ref=sums.at[me], send_sem=sum_send.at[p], recv_sem=sum_recv.at[me],
            device_id=device, device_id_type=MESH,
        )
        copy.start()
        exchanges.append(copy)
    sent = list(exchanges)
    for e in range(len(EARLY)):
        for way in range(2):
            copy = early(way, e)
            copy.start()
            sent.append(copy)
    sums[pl.ds(me, 1)] = msg[...][None]
    arrivals = []
    for device, p in fsdp_peers():
        arrivals.append(pltpu.make_async_remote_copy(
            src_ref=msg, dst_ref=sums.at[p], send_sem=sum_send.at[p], recv_sem=sum_recv.at[p],
            device_id=device, device_id_type=MESH,
        ))
    for copy in arrivals:
        copy.wait_recv()

    total = sums[0]
    for s in range(1, SHARDS):
        total = total + sums[s]
    scale = jnp.sqrt(total)
    inverse = 1.0 / scale

    def put(shard, a, h, read):
        rows = pl.ds(pl.multiple_of(shard * ROWS + h * HALF, HALF), HALF)
        for j in range(2):
            lanes = pl.ds(j * LANES, LANES)
            value = read(lanes) * inverse[2 * a + j : 2 * a + j + 1]
            outs[a][rows, lanes] = value.astype(jnp.bfloat16)

    for a, h in sorted(((a, h) for a in range(3) for h in range(2)), key=lambda piece: piece in EARLY):
        put(me, a, h, lambda lanes: mixed[a, pl.ds(h * HALF, HALF), lanes])

    for a in range(3):
        for h in range(2):
            if (a, h) in EARLY:
                continue
            for way in range(2):
                copy = hop(way, 2 * a + h, me, a, h)
                copy.start()
                sent.append(copy)
    for a in range(3):
        for h in range(2):
            copy = across(own_send.at[2 * a + h], own_recv.at[2 * a + h], me, a, h)
            copy.start()
            sent.append(copy)

    for a, ref in enumerate((scale_q, scale_k, scale_v)):
        for j in range(2):
            ref[:, pl.ds(j * LANES, LANES)] = scale[2 * a + j : 2 * a + j + 1]

    for s in range(SHARDS):
        plane_out[pl.ds(s, 1), :] = sums[s, 6:7, :]
    def to_root(p):
        return pltpu.make_async_remote_copy(
            src_ref=plane_out, dst_ref=plane_in.at[p], send_sem=plane_send, recv_sem=plane_recv.at[p],
            device_id={"cols_0": 0, "cols_1": 0}, device_id_type=MESH,
        )

    def answer(device, p):
        return pltpu.make_async_remote_copy(
            src_ref=norm_f32, dst_ref=norm_f32, send_sem=answer_send.at[p], recv_sem=answer_recv,
            device_id=device, device_id_type=MESH,
        )

    @pl.when(col > 0)
    def _():
        to_root(col).start()

    def answer_all():
        plane_in[0] = plane_out[...]
        for _, p in plane_peers():
            to_root(p).wait_recv()
        for side in range(2):
            gathered = plane_in[8 * side]
            for k in range(1, 8):
                gathered = gathered + plane_in[8 * side + k]
            norm_f32[pl.ds(side, SHARDS, stride=2), :] = gathered
        for device, p in plane_peers():
            answer(device, p).start()

    for i in range(STEPS):
        if i == ANSWER:
            pl.when(col == 0)(answer_all)
        for way in range(2):
            d, a, h = STREAM[way][i]
            shard, _, _ = along(way, i)
            if d == 1 and (a, h) in EARLY:
                e = EARLY.index((a, h))
                early(way, e).wait_recv()
                put(shard, a, h, lambda lanes: landed[way, e, :, lanes])
            else:
                hop(way, i, shard, a, h).wait_recv()
            if (d + 1, a, h) in STREAM[way]:
                copy = hop(way, STREAM[way].index((d + 1, a, h)), shard, a, h)
                copy.start()
                sent.append(copy)
            copy = across(d2d_send.at[way, i], d2d_recv.at[way, i], shard, a, h)
            copy.start()
            sent.append(copy)

    @pl.when(col > 0)
    def _():
        answer({"cols_0": 0, "cols_1": 0}, 0).wait_recv()
        to_root(col).wait_send()

    norm[...] = norm_f32[...].astype(jnp.bfloat16)

    @pl.when(col == 0)
    def _():
        for device, p in plane_peers():
            answer(device, p).wait_send()

    partner = z * CORES + 1 - c
    for a in range(3):
        for h in range(2):
            across(own_send.at[2 * a + h], own_recv.at[2 * a + h], partner, a, h).wait_recv()
    for i in range(STEPS):
        for way in range(2):
            shard, a, h = along(way, i)
            across(d2d_send.at[way, i], d2d_recv.at[way, i], shard + 1 - 2 * c, a, h).wait_recv()
    for copy in sent:
        copy.wait_send()


PARTS = 4


def store_kernel(*refs):
    ins, outs, sem = refs[:7], refs[7:14], refs[14]
    copies = []
    for i, (src, dst) in enumerate(zip(ins, outs)):
        parts = PARTS if i < 3 else 1
        rows = src.shape[0] // parts
        for p in range(parts):
            window = pl.ds(p * rows, rows)
            copies.append(pltpu.make_async_copy(src.at[window], dst.at[window], sem.at[len(copies)]))
    for copy in copies:
        copy.start()
    for copy in copies:
        copy.wait()


def store(arrays):
    return pl.pallas_call(
        store_kernel,
        name="store",
        out_shape=tuple(jax.ShapeDtypeStruct(a.shape, a.dtype) for a in arrays),
        in_specs=[pl.BlockSpec(memory_space=pltpu.VMEM)] * 7,
        out_specs=(pl.BlockSpec(memory_space=pltpu.HBM),) * 7,
        scratch_shapes=[pltpu.SemaphoreType.DMA((3 * PARTS + 4,))],
        compiler_params=pltpu.CompilerParams(vmem_limit_bytes=16 * 2**20),
    )(*arrays)


def per_device(oq, tq, ok, tk, ov, tv, share, train, step):
    f32, bf16 = jnp.float32, jnp.bfloat16
    whole = jax.ShapeDtypeStruct((SHARDS * ROWS, 2 * LANES), bf16)
    scale = jax.ShapeDtypeStruct((1, 2 * LANES), f32)
    vmem = pl.BlockSpec(memory_space=pltpu.VMEM)
    dma = pltpu.SemaphoreType.DMA
    outs = pl.pallas_call(
        kernel,
        name="mix_and_gather",
        out_shape=(whole, whole, whole, scale, scale, scale, jax.ShapeDtypeStruct((32, LANES), bf16)),
        in_specs=[pl.BlockSpec(memory_space=pltpu.HBM)] * 9,
        out_specs=(vmem,) * 7,
        scratch_shapes=[
            pltpu.VMEM((6, ROWS, 2 * LANES), f32),
            pltpu.VMEM((1, ROWS), f32),
            pltpu.VMEM((2, 1, PIECE), f32),
            pltpu.VMEM((3, ROWS, 2 * LANES), f32),
            pltpu.VMEM((2, len(EARLY), HALF, 2 * LANES), f32),
            pltpu.VMEM((8, LANES), f32),
            pltpu.VMEM((SHARDS, 8, LANES), f32),
            pltpu.VMEM((SHARDS, LANES), f32),
            pltpu.VMEM((PLANE, SHARDS, LANES), f32),
            pltpu.VMEM((32, LANES), f32),
            dma((9,)),
            dma((SHARDS,)),
            dma((SHARDS,)),
            dma,
            dma((PLANE,)),
            dma((PLANE,)),
            dma,
            dma((2, STEPS)),
            dma((2, STEPS)),
            dma((6,)),
            dma((6,)),
            dma((2, STEPS)),
            dma((2, STEPS)),
        ],
        compiler_params=pltpu.CompilerParams(collective_id=0, has_side_effects=True, vmem_limit_bytes=24 * 2**20),
    )(*(pltpu.with_memory_space_constraint(a, pltpu.HBM) for a in (
        oq, tq, ok, tk, ov, tv, share.reshape(1, -1), train.reshape(1, -1), step.reshape(1, -1)
    )))
    q, k, v, scale_q, scale_k, scale_v, norm = store(outs)
    return q, k, v, scale_q.reshape(-1), scale_k.reshape(-1), scale_v.reshape(-1), norm.reshape(-1)


def solution(mesh):
    split = Mesh(mesh.devices.reshape(Z, CORES, PLANE_Y, PLANE_X), FSDP_COLS)
    block = P(FSDP, COLS)
    return jax.shard_map(
        per_device,
        mesh=split,
        in_specs=(block,) * 6 + (P(FSDP), P(FSDP_COLS), P(FSDP_COLS)),
        out_specs=(P(None, COLS),) * 3 + (P(COLS),) * 3 + (P(),),
        check_vma=False,
    )
```

```python
import functools

import jax
import jax.numpy as jnp
from jax import lax
from jax.experimental import pallas as pl
from jax.experimental.pallas import tpu as pltpu
from jax.sharding import Mesh
from jax.sharding import PartitionSpec as P

FSDP = ("fsdp_0", "fsdp_1")
FSDP_COLS = ("fsdp_0", "fsdp_1", "cols_0", "cols_1")
COLS = ("cols_0", "cols_1")
MESH = pl.DeviceIdType.MESH

Z = 8
CORES = 2
SHARDS = Z * CORES
PLANE_Y = 4
PLANE_X = 4
PLANE = PLANE_Y * PLANE_X
ROWS = 256
HALF = 128
LANES = 128
PIECE = 16

EARLY = [(0, 0, 128), (0, 128, 64)]
EARLY_ROWS = sum(n for _, _, n in EARLY)
LATE = [(0, EARLY_ROWS, ROWS - EARLY_ROWS), (1, 0, ROWS), (2, 0, ROWS)]
WHOLE = [(a, 0, ROWS) for a in range(3)]
CROSS = (0, HALF)
BASE = tuple(
    [(1, p) for p in EARLY + LATE]
    + [(2, p) for p in WHOLE]
    + [(3, p) for p in WHOLE[:2] + [(2, CROSS[way], HALF), (2, CROSS[1 - way], HALF)]]
    for way in (0, 1)
)
STEPS = len(BASE[0])
LAST = [(a, other) for a in range(3) for other in (0, 1)]
TAIL = len(LAST)
ANSWER = 5
LAG = 1
PARTS = 4


def kernel(
    oq, tq, ok, tk, ov, tv, share, train, step,
    out_q, out_k, out_v, scale_q, scale_k, scale_v, norm,
    ins, share_v, norm_in, mixed, landed, msg, sums, plane_out, plane_in, norm_f32,
    in_sem, sum_send, sum_recv, plane_send, plane_recv, answer_send, answer_recv,
    early_send, ici_send, ici_recv, push_send, push_recv, cross_recv,
):
    z, c = lax.axis_index("fsdp_0"), lax.axis_index("fsdp_1")
    col = lax.axis_index("cols_0") * PLANE_X + lax.axis_index("cols_1")
    me = z * CORES + c
    outs = (out_q, out_k, out_v)

    def fsdp_peers():
        for dz in (4, 5, 3, 6, 2, 7, 1, 0):
            for dc in (0, 1):
                if dz or dc:
                    pz, pc = lax.rem(z + dz, Z), lax.rem(c + dc, CORES)
                    yield {"fsdp_0": pz, "fsdp_1": pc}, pz * CORES + pc

    def plane_peers():
        for p in range(1, PLANE):
            yield {"cols_0": p // PLANE_X, "cols_1": p % PLANE_X}, p

    barrier = pltpu.get_barrier_semaphore()
    for device, _ in fsdp_peers():
        pl.semaphore_signal(barrier, inc=1, device_id=device, device_id_type=MESH)

    pltpu.make_async_copy(share, share_v, in_sem.at[3]).start()
    for i, src in enumerate((oq, tq, ok, tk, ov, tv)):
        pltpu.make_async_copy(src, ins.at[i], in_sem.at[i // 2]).start()
    for i, src in enumerate((train, step)):
        pltpu.make_async_copy(src, norm_in.at[i], in_sem.at[4]).start()

    @pl.when(col == 0)
    def _():
        for device, _ in plane_peers():
            pl.semaphore_signal(barrier, inc=1, device_id=device, device_id_type=MESH)

    def place(shard, piece):
        a, r, n = piece
        return outs[a].at[pl.ds(pl.multiple_of(shard * ROWS + r, n), n)]

    def shard_of(way, d, core):
        return lax.rem(z + (Z - d if way == 0 else d), Z) * CORES + core

    def hop(way, i, src, dst, send):
        target = lax.rem(z + (1 if way == 0 else Z - 1), Z)
        return pltpu.make_async_remote_copy(
            src_ref=src, dst_ref=dst, send_sem=send, recv_sem=ici_recv.at[way, i],
            device_id={"fsdp_0": target}, device_id_type=MESH,
        )

    def early(way, i):
        a, r, n = EARLY[i]
        return hop(way, i, mixed.at[a, pl.ds(r, n)], landed.at[way, pl.ds(r, n)], early_send)

    def ring(way, i, shard):
        piece = BASE[way][i][1]
        ref = place(shard, piece)
        return hop(way, i, ref, ref, ici_send.at[piece[0]])

    def last(way, t, d):
        a, other = LAST[t]
        core = lax.rem(c + other, CORES)
        ref = place(shard_of(way, d, core), (a, CROSS[way], HALF))
        return hop(way, STEPS + t, ref, ref, ici_send.at[a])

    def across(ref, a, recv):
        return pltpu.make_async_remote_copy(
            src_ref=ref, dst_ref=ref, send_sem=push_send.at[a], recv_sem=recv,
            device_id={"fsdp_1": 1 - c}, device_id_type=MESH,
        )

    def push(shard, piece):
        return across(place(shard, piece), piece[0], push_recv.at[piece[0]])

    def rows_of(a, rows):
        return outs[a].at[pl.ds(0, rows)]

    msg[...] = jnp.zeros_like(msg)
    pltpu.make_async_copy(share, share_v, in_sem.at[3]).wait()
    shares = [
        jnp.broadcast_to(share_v[:, r * HALF : (r + 1) * HALF], (LANES, HALF)).T for r in range(2)
    ]
    for a in range(3):
        pair = ins.at[pl.ds(2 * a, 2)]
        pltpu.make_async_copy(pair, pair, in_sem.at[a]).wait()
        for j in range(2):
            lanes = pl.ds(j * LANES, LANES)
            total = jnp.zeros((1, LANES), jnp.float32)
            for r in range(2):
                rows = pl.ds(r * HALF, HALF)
                value = shares[r] * ins[2 * a, rows, lanes] + (1.0 - shares[r]) * ins[2 * a + 1, rows, lanes]
                mixed[a, rows, lanes] = value
                total = total + jnp.sum(value * value, axis=0, keepdims=True)
            msg[pl.ds(2 * a + j, 1), :] = total
    pltpu.make_async_copy(norm_in, norm_in, in_sem.at[4]).wait()
    piece = jnp.concatenate(
        [norm_in[0] + norm_in[1], jnp.zeros((1, LANES - PIECE), jnp.float32)], axis=1
    )
    piece = pltpu.roll(jnp.broadcast_to(piece, (8, LANES)), lax.rem(col, 8) * PIECE, 1)
    msg[pl.ds(6, 1), :] = piece[:1]

    pl.semaphore_wait(barrier, SHARDS - 1 + (col + PLANE - 1) // PLANE)

    def message(device, slot):
        return pltpu.make_async_remote_copy(
            src_ref=msg, dst_ref=sums.at[slot], send_sem=sum_send, recv_sem=sum_recv,
            device_id=device, device_id_type=MESH,
        )

    for device, _ in fsdp_peers():
        message(device, me).start()
    for i in range(len(EARLY)):
        for way in range(2):
            early(way, i).start()
    sums[pl.ds(me, 1)] = msg[...][None]

    def all_messages(slots):
        return pltpu.make_async_remote_copy(
            src_ref=slots, dst_ref=slots, send_sem=sum_send, recv_sem=sum_recv,
            device_id={"fsdp_1": 1 - c}, device_id_type=MESH,
        )

    all_messages(sums.at[pl.ds(0, SHARDS - 1)]).wait_recv()

    total = sums[0]
    for s in range(1, SHARDS):
        total = total + sums[s]
    scale = jnp.sqrt(total)
    inverse = 1.0 / scale

    def put(shard, piece, read):
        a, r, n = piece
        rows = pl.ds(pl.multiple_of(shard * ROWS + r, n), n)
        for j in range(2):
            lanes = pl.ds(j * LANES, LANES)
            value = read(lanes) * inverse[2 * a + j : 2 * a + j + 1]
            outs[a][rows, lanes] = value.astype(jnp.bfloat16)

    for piece in LATE + EARLY:
        a, r, n = piece
        put(me, piece, lambda lanes: mixed[a, pl.ds(r, n), lanes])
    for i in range(len(EARLY), len(EARLY + LATE)):
        for way in range(2):
            ring(way, i, me).start()
    for piece in WHOLE:
        push(me, piece).start()

    for a, ref in enumerate((scale_q, scale_k, scale_v)):
        for j in range(2):
            ref[:, pl.ds(j * LANES, LANES)] = scale[2 * a + j : 2 * a + j + 1]

    for s in range(SHARDS):
        plane_out[pl.ds(s, 1), :] = sums[s, 6:7, :]

    def to_root(p):
        return pltpu.make_async_remote_copy(
            src_ref=plane_out, dst_ref=plane_in.at[p], send_sem=plane_send, recv_sem=plane_recv,
            device_id={"cols_0": 0, "cols_1": 0}, device_id_type=MESH,
        )

    def answer(device):
        return pltpu.make_async_remote_copy(
            src_ref=norm_f32, dst_ref=norm_f32, send_sem=answer_send, recv_sem=answer_recv,
            device_id=device, device_id_type=MESH,
        )

    @pl.when(col > 0)
    def _():
        to_root(col).start()

    def answer_all():
        plane_in[0] = plane_out[...]
        pieces = plane_in.at[pl.ds(1, PLANE - 1)]
        pltpu.make_async_remote_copy(
            src_ref=pieces, dst_ref=pieces, send_sem=plane_send, recv_sem=plane_recv,
            device_id={"cols_0": 0, "cols_1": 1}, device_id_type=MESH,
        ).wait_recv()
        for side in range(2):
            gathered = plane_in[8 * side]
            for k in range(1, 8):
                gathered = gathered + plane_in[8 * side + k]
            norm_f32[pl.ds(side, SHARDS, stride=2), :] = gathered
        for device, _ in plane_peers():
            answer(device).start()

    def onward(way, i):
        d, (a, r, n) = BASE[way][i]
        if d == 1 and r + n == ROWS or d == 2:
            for k, (far, piece) in enumerate(BASE[way]):
                if far == d + 1 and piece[0] == a:
                    ring(way, k, shard_of(way, d, c)).start()

    def crosses(way, i):
        d, (a, r, n) = BASE[way][i]
        return d == 3 and r <= CROSS[way] < r + n

    def from_partner(way, i):
        _, piece = BASE[way][i]
        a = piece[0]
        across(place(shard_of(way, 3, 1 - c), piece), a, cross_recv.at[way, a]).wait_recv()
        last(way, LAST.index((a, 1)), 3).start()

    for i in range(STEPS + LAG):
        if i == ANSWER:
            pl.when(col == 0)(answer_all)
        if i < STEPS:
            for way in range(2):
                d, piece = BASE[way][i]
                a = piece[0]
                shard = shard_of(way, d, c)
                if d == 1 and piece in EARLY:
                    early(way, i).wait_recv()
                    put(shard, piece, lambda lanes: landed[way, pl.ds(piece[1], piece[2]), lanes])
                else:
                    ring(way, i, shard).wait_recv()
                onward(way, i)
                if crosses(way, i):
                    @pl.when(c == 1)
                    def _():
                        last(way, LAST.index((a, 0)), 3).start()
                        push(shard, piece).start()

                    @pl.when(c == 0)
                    def _():
                        across(place(shard, piece), a, cross_recv.at[way, a]).start()
                else:
                    push(shard, piece).start()
        for way in range(2):
            if i >= LAG and crosses(way, i - LAG):
                pl.when(c == 1)(functools.partial(from_partner, way, i - LAG))

    @pl.when(c == 1)
    def _():
        for t, (a, other) in enumerate(LAST):
            for way in range(2):
                last(way, t, 4).wait_recv()
                push(shard_of(way, 4, lax.rem(c + other, CORES)), (a, CROSS[way], HALF)).start()

    @pl.when(col > 0)
    def _():
        answer({"cols_0": 0, "cols_1": 0}).wait_recv()
        to_root(col).wait_send()

    norm[...] = norm_f32[...].astype(jnp.bfloat16)

    @pl.when(col == 0)
    def _():
        ref = ins.at[0, pl.ds(0, 16 * (PLANE - 1))]
        pltpu.make_async_remote_copy(
            src_ref=ref, dst_ref=ref, send_sem=answer_send, recv_sem=answer_recv,
            device_id={"cols_0": 0, "cols_1": 1}, device_id_type=MESH,
        ).wait_send()

    all_messages(sums.at[pl.ds(0, SHARDS - 1)]).wait_send()
    ref = ins.at[pl.ds(0, 2), pl.ds(0, EARLY_ROWS)]
    hop(0, 0, ref, ref, early_send).wait_send()

    def finish(core):
        def _():
            for a in range(3):
                own = ROWS - (EARLY_ROWS if a == 0 else 0)
                ring_rows = 2 * (own + 2 * ROWS + (ROWS if core else 0))
                pushed = ROWS + 2 * (3 * ROWS + (ROWS if core else 0))
                crossing = sum(p[2] for way in (0, 1) for i, (_, p) in enumerate(BASE[way]) if crosses(way, i) and p[0] == a)
                come = ROWS + 2 * 3 * ROWS + (-crossing if core else 2 * ROWS)
                ref = rows_of(a, come)
                across(ref, a, push_recv.at[a]).wait_recv()
                ref = rows_of(a, ring_rows)
                hop(0, 0, ref, ref, ici_send.at[a]).wait_send()
                ref = rows_of(a, pushed)
                across(ref, a, push_recv.at[a]).wait_send()

        return _

    for core in range(CORES):
        pl.when(c == core)(finish(core))


def store_kernel(*refs):
    ins, outs, sem = refs[:7], refs[7:14], refs[14]
    for i, (src, dst) in enumerate(zip(ins, outs)):
        parts = PARTS if i < 3 else 1
        rows = src.shape[0] // parts
        for p in range(parts):
            window = pl.ds(p * rows, rows)
            pltpu.make_async_copy(src.at[window], dst.at[window], sem.at[i]).start()
    for i, (src, dst) in enumerate(zip(ins, outs)):
        pltpu.make_async_copy(src, dst, sem.at[i]).wait()


def store(arrays):
    return pl.pallas_call(
        store_kernel,
        name="store",
        out_shape=tuple(jax.ShapeDtypeStruct(a.shape, a.dtype) for a in arrays),
        in_specs=[pl.BlockSpec(memory_space=pltpu.VMEM)] * 7,
        out_specs=(pl.BlockSpec(memory_space=pltpu.HBM),) * 7,
        scratch_shapes=[pltpu.SemaphoreType.DMA((7,))],
        compiler_params=pltpu.CompilerParams(vmem_limit_bytes=16 * 2**20),
    )(*arrays)


def per_device(oq, tq, ok, tk, ov, tv, share, train, step):
    f32, bf16 = jnp.float32, jnp.bfloat16
    whole = jax.ShapeDtypeStruct((SHARDS * ROWS, 2 * LANES), bf16)
    scale = jax.ShapeDtypeStruct((1, 2 * LANES), f32)
    vmem = pl.BlockSpec(memory_space=pltpu.VMEM)
    dma = pltpu.SemaphoreType.DMA
    outs = pl.pallas_call(
        kernel,
        name="mix_and_gather",
        out_shape=(whole, whole, whole, scale, scale, scale, jax.ShapeDtypeStruct((32, LANES), bf16)),
        in_specs=[pl.BlockSpec(memory_space=pltpu.HBM)] * 9,
        out_specs=(vmem,) * 7,
        scratch_shapes=[
            pltpu.VMEM((6, ROWS, 2 * LANES), f32),
            pltpu.VMEM((1, ROWS), f32),
            pltpu.VMEM((2, 1, PIECE), f32),
            pltpu.VMEM((3, ROWS, 2 * LANES), f32),
            pltpu.VMEM((2, EARLY_ROWS, 2 * LANES), f32),
            pltpu.VMEM((8, LANES), f32),
            pltpu.VMEM((SHARDS, 8, LANES), f32),
            pltpu.VMEM((SHARDS, LANES), f32),
            pltpu.VMEM((PLANE, SHARDS, LANES), f32),
            pltpu.VMEM((32, LANES), f32),
            dma((5,)),
            dma,
            dma,
            dma,
            dma,
            dma,
            dma,
            dma,
            dma((3,)),
            dma((2, STEPS + TAIL)),
            dma((3,)),
            dma((3,)),
            dma((2, 3)),
        ],
        compiler_params=pltpu.CompilerParams(
            collective_id=0, has_side_effects=True, vmem_limit_bytes=24 * 2**20
        ),
    )(*(pltpu.with_memory_space_constraint(a, pltpu.HBM) for a in (
        oq, tq, ok, tk, ov, tv, share.reshape(1, -1), train.reshape(1, -1), step.reshape(1, -1)
    )))
    q, k, v, scale_q, scale_k, scale_v, norm = store(outs)
    return q, k, v, scale_q.reshape(-1), scale_k.reshape(-1), scale_v.reshape(-1), norm.reshape(-1)


def solution(mesh):
    split = Mesh(mesh.devices.reshape(Z, CORES, PLANE_Y, PLANE_X), FSDP_COLS)
    block = P(FSDP, COLS)
    return jax.shard_map(
        per_device,
        mesh=split,
        in_specs=(block,) * 6 + (P(FSDP), P(FSDP_COLS), P(FSDP_COLS)),
        out_specs=(P(None, COLS),) * 3 + (P(COLS),) * 3 + (P(),),
        check_vma=False,
    )
```

```python
import functools
import math

import jax
import jax.numpy as jnp
from jax import lax
from jax.experimental import pallas as pl
from jax.experimental.pallas import tpu as pltpu
from jax.sharding import Mesh
from jax.sharding import PartitionSpec as P

FSDP = ("fsdp_0", "fsdp_1")
FSDP_COLS = ("fsdp_0", "fsdp_1", "cols_0", "cols_1")
COLS = ("cols_0", "cols_1")
MESH = pl.DeviceIdType.MESH

Z = 8
CORES = 2
SHARDS = Z * CORES
PLANE_Y = 4
PLANE_X = 4
PLANE = PLANE_Y * PLANE_X
ROWS = 256
HALF = 128
LANES = 128
PIECE = 16

WHOLE = [(a, 0, ROWS) for a in range(3)]
FIRST = (
    [(0, 0, ROWS), (1, 0, ROWS), (2, 0, ROWS)],
    [(0, 0, HALF), (0, HALF, HALF), (1, 0, ROWS), (2, 0, ROWS)],
)
EARLY = (1, 1)
SPLIT = 128
CROSS = ((0, SPLIT), (SPLIT, ROWS - SPLIT))
BASE = tuple(
    [(1, p) for p in range(max(len(f) for f in FIRST))]
    + [(2, p) for p in WHOLE]
    + [(3, p) for p in WHOLE[:2] + [(2, *CROSS[way]), (2, *CROSS[1 - way])]]
    for way in (0, 1)
)
NEAR = sum(d == 1 for d, _ in BASE[0])
EARLY_AT = [[sum(n for _, _, n in f[:i]) for i in range(e + 1)] for f, e in zip(FIRST, EARLY)]
EARLY_ROWS = max(at[-1] for at in EARLY_AT)
STEPS = len(BASE[0])
LAST = [(a, other) for a in range(3) for other in (0, 1)]
TAIL = len(LAST)
ANSWER = 4
PASS = 7
LAG = 1
PARTS = 4


def kernel(
    oq, tq, ok, tk, ov, tv, share, train, step,
    out_q, out_k, out_v, scale_q, scale_k, scale_v, norm,
    ins, share_v, norm_in, mixed, landed, msg, both, total_v, sums, plane_out, plane_in, norm_f32,
    in_sem, chip_send, chip_recv, sum_send, sum_recv, plane_send, plane_recv, answer_send, answer_recv,
    early_send, ici_send, ici_recv, push_send, push_recv, cross_recv,
):
    z, c = lax.axis_index("fsdp_0"), lax.axis_index("fsdp_1")
    col = lax.axis_index("cols_0") * PLANE_X + lax.axis_index("cols_1")
    me = z * CORES + c
    outs = (out_q, out_k, out_v)

    ahead, behind = lax.rem(z + 1, Z), lax.rem(z + Z - 1, Z)
    partner = {"fsdp_1": 1 - c}

    def far_peers():
        for dz in (4, 5, 3, 6, 2, 7, 1):
            yield {"fsdp_0": lax.rem(z + dz, Z)}

    def plane_peers():
        for p in range(1, PLANE):
            yield {"cols_0": p // PLANE_X, "cols_1": p % PLANE_X}

    barrier = pltpu.get_barrier_semaphore()

    def greet(device):
        pl.semaphore_signal(barrier, inc=1, device_id=device, device_id_type=MESH)

    @pl.when(c == 0)
    def _():
        for target in (ahead, behind):
            greet({"fsdp_0": target})

    @pl.when(c == 1)
    def _():
        for device in far_peers():
            greet(device)

    greet(partner)

    pltpu.make_async_copy(share, share_v, in_sem.at[3]).start()
    for i, src in enumerate((oq, tq, ok, tk, ov, tv)):
        pltpu.make_async_copy(src, ins.at[i], in_sem.at[i // 2]).start()
    for i, src in enumerate((train, step)):
        pltpu.make_async_copy(src, norm_in.at[i], in_sem.at[4]).start()

    @pl.when(c * PLANE + col == PLANE)
    def _():
        for device in plane_peers():
            greet(device)

    def place(shard, piece):
        a, r, n = piece
        return outs[a].at[pl.ds(pl.multiple_of(shard * ROWS + r, math.gcd(ROWS, r, n)), n)]

    def shard_of(way, d, core):
        return lax.rem(z + (Z - d if way == 0 else d), Z) * CORES + core

    def hop(way, i, src, dst, send):
        target = ahead if way == 0 else behind
        return pltpu.make_async_remote_copy(
            src_ref=src, dst_ref=dst, send_sem=send, recv_sem=ici_recv.at[way, i],
            device_id={"fsdp_0": target}, device_id_type=MESH,
        )

    def early(way, i, core):
        a, r, n = FIRST[core][i]
        return hop(way, i, mixed.at[a, pl.ds(r, n)], landed.at[way, pl.ds(EARLY_AT[core][i], n)], early_send)

    def ring(way, i, shard):
        piece = BASE[way][i][1]
        ref = place(shard, piece)
        return hop(way, i, ref, ref, ici_send.at[piece[0]])

    def first(way, i, core, shard):
        piece = FIRST[core][i]
        ref = place(shard, piece)
        return hop(way, i, ref, ref, ici_send.at[piece[0]])

    def last(way, t, d):
        a, other = LAST[t]
        core = lax.rem(c + other, CORES)
        ref = place(shard_of(way, d, core), (a, *CROSS[way]))
        return hop(way, STEPS + t, ref, ref, ici_send.at[a])

    def across(ref, a, recv):
        return pltpu.make_async_remote_copy(
            src_ref=ref, dst_ref=ref, send_sem=push_send.at[a], recv_sem=recv,
            device_id=partner, device_id_type=MESH,
        )

    def push(shard, piece):
        return across(place(shard, piece), piece[0], push_recv.at[piece[0]])

    def rows_of(a, rows):
        return outs[a].at[pl.ds(0, rows)]

    msg[...] = jnp.zeros_like(msg)
    pltpu.make_async_copy(share, share_v, in_sem.at[3]).wait()
    shares = [
        jnp.broadcast_to(share_v[:, r * HALF : (r + 1) * HALF], (LANES, HALF)).T for r in range(2)
    ]
    for a in range(3):
        pair = ins.at[pl.ds(2 * a, 2)]
        pltpu.make_async_copy(pair, pair, in_sem.at[a]).wait()
        for j in range(2):
            lanes = pl.ds(j * LANES, LANES)
            total = jnp.zeros((1, LANES), jnp.float32)
            for r in range(2):
                rows = pl.ds(r * HALF, HALF)
                value = shares[r] * ins[2 * a, rows, lanes] + (1.0 - shares[r]) * ins[2 * a + 1, rows, lanes]
                mixed[a, rows, lanes] = value
                total = total + jnp.sum(value * value, axis=0, keepdims=True)
            msg[pl.ds(2 * a + j, 1), :] = total
    pltpu.make_async_copy(norm_in, norm_in, in_sem.at[4]).wait()
    piece = jnp.concatenate(
        [norm_in[0] + norm_in[1], jnp.zeros((1, LANES - PIECE), jnp.float32)], axis=1
    )
    piece = pltpu.roll(jnp.broadcast_to(piece, (8, LANES)), lax.rem(col, 8) * PIECE, 1)
    msg[pl.ds(6 + c, 1), :] = piece[:1]

    def over_chip(src, dst):
        return pltpu.make_async_remote_copy(
            src_ref=src, dst_ref=dst, send_sem=chip_send, recv_sem=chip_recv,
            device_id=partner, device_id_type=MESH,
        )

    def message(device, src, slot):
        return pltpu.make_async_remote_copy(
            src_ref=src, dst_ref=slot, send_sem=sum_send, recv_sem=sum_recv,
            device_id=device, device_id_type=MESH,
        )

    every = sums.at[pl.ds(0, Z - 1)]

    @pl.when(c == 0)
    def _():
        pl.semaphore_wait(barrier, 3)
        over_chip(msg, both).start()
        for i in range(EARLY[0]):
            for way in range(2):
                early(way, i, 0).start()
        over_chip(total_v, total_v).wait_recv()

    @pl.when(c == 1)
    def _():
        pl.semaphore_wait(barrier, Z + (col + PLANE - 1) // PLANE)
        over_chip(msg, both).wait_recv()
        both[...] = both[...] + msg[...]
        for device in far_peers():
            message(device, both, sums.at[z]).start()
        for i in range(EARLY[1]):
            for way in range(2):
                early(way, i, 1).start()
        sums[pl.ds(z, 1)] = both[...][None]
        message(partner, every, every).wait_recv()
        total = sums[0]
        for s in range(1, Z):
            total = total + sums[s]
        total_v[...] = total
        over_chip(total_v, total_v).start()

    scale = jnp.sqrt(total_v[...])
    inverse = 1.0 / scale

    def put(shard, piece, read):
        a, r, n = piece
        rows = pl.ds(pl.multiple_of(shard * ROWS + r, math.gcd(ROWS, r, n)), n)
        for j in range(2):
            lanes = pl.ds(j * LANES, LANES)
            value = read(lanes) * inverse[2 * a + j : 2 * a + j + 1]
            outs[a][rows, lanes] = value.astype(jnp.bfloat16)

    def put_own(piece):
        a, r, n = piece
        put(me, piece, lambda lanes: mixed[a, pl.ds(r, n), lanes])

    for piece in WHOLE:
        put_own(piece)
    for core in range(CORES):
        @pl.when(c == core)
        def _():
            for i in range(EARLY[core], len(FIRST[core])):
                for way in range(2):
                    first(way, i, core, me).start()

    for piece in WHOLE:
        push(me, piece).start()

    for a, ref in enumerate((scale_q, scale_k, scale_v)):
        for j in range(2):
            ref[:, pl.ds(j * LANES, LANES)] = scale[2 * a + j : 2 * a + j + 1]

    def to_root():
        return pltpu.make_async_remote_copy(
            src_ref=plane_out, dst_ref=plane_in.at[col], send_sem=plane_send, recv_sem=plane_recv,
            device_id={"cols_0": 0, "cols_1": 0}, device_id_type=MESH,
        )

    def answer(device):
        return pltpu.make_async_remote_copy(
            src_ref=norm_f32, dst_ref=norm_f32, send_sem=answer_send, recv_sem=answer_recv,
            device_id=device, device_id_type=MESH,
        )

    @pl.when(c == 1)
    def _():
        for s in range(SHARDS):
            plane_out[pl.ds(s, 1), :] = sums[s // CORES, 6 + s % CORES : 7 + s % CORES, :]

    @pl.when((col > 0) & (c == 1))
    def _():
        to_root().start()

    def answer_all():
        plane_in[0] = plane_out[...]
        pieces = plane_in.at[pl.ds(1, PLANE - 1)]
        pltpu.make_async_remote_copy(
            src_ref=pieces, dst_ref=pieces, send_sem=plane_send, recv_sem=plane_recv,
            device_id={"cols_0": 0, "cols_1": 1}, device_id_type=MESH,
        ).wait_recv()
        for side in range(2):
            gathered = plane_in[8 * side]
            for k in range(1, 8):
                gathered = gathered + plane_in[8 * side + k]
            norm_f32[pl.ds(side, SHARDS, stride=2), :] = gathered
        for device in plane_peers():
            answer(device).start()
        answer(partner).start()

    def pass_on():
        answer({"cols_0": 0, "cols_1": 0}).wait_recv()
        answer(partner).start()

    def onward(way, i):
        d, piece = BASE[way][i]
        if d == 2:
            go_on(way, piece[0], 2)

    def go_on(way, a, d):
        for k, (far, piece) in enumerate(BASE[way]):
            if far == d + 1 and piece[0] == a:
                ring(way, k, shard_of(way, d, c)).start()

    def crosses(way, i):
        d, piece = BASE[way][i]
        return d == 3 and piece[1] <= CROSS[way][0] < piece[1] + piece[2]

    def from_partner(way, i):
        _, piece = BASE[way][i]
        a = piece[0]
        across(place(shard_of(way, 3, 1 - c), piece), a, cross_recv.at[way, a]).wait_recv()
        last(way, LAST.index((a, 1)), 3).start()

    def near(way, i, core):
        piece = FIRST[core][i]
        a, r, n = piece
        shard = shard_of(way, 1, core)
        if i < EARLY[core]:
            early(way, i, core).wait_recv()
            put(shard, piece, lambda lanes: landed[way, pl.ds(EARLY_AT[core][i], n), lanes])
        else:
            first(way, i, core, shard).wait_recv()
        if r + n == ROWS:
            go_on(way, a, 1)
        push(shard, piece).start()

    for i in range(STEPS + LAG):
        if i == ANSWER:
            pl.when(c * PLANE + col == PLANE)(answer_all)
        if i == PASS:
            pl.when((col > 0) & (c == 1))(pass_on)
        if i < STEPS:
            for way in range(2):
                d, piece = BASE[way][i]
                if d == 1:
                    for core in range(CORES):
                        if i < len(FIRST[core]):
                            pl.when(c == core)(functools.partial(near, way, i, core))
                    continue
                a = piece[0]
                shard = shard_of(way, d, c)
                ring(way, i, shard).wait_recv()
                onward(way, i)
                if crosses(way, i):
                    @pl.when(c == 1)
                    def _():
                        last(way, LAST.index((a, 0)), 3).start()
                        push(shard, piece).start()

                    @pl.when(c == 0)
                    def _():
                        across(place(shard, piece), a, cross_recv.at[way, a]).start()
                else:
                    push(shard, piece).start()
        for way in range(2):
            if i >= LAG and crosses(way, i - LAG):
                pl.when(c == 1)(functools.partial(from_partner, way, i - LAG))

    @pl.when(c == 1)
    def _():
        for t, (a, other) in enumerate(LAST):
            for way in range(2):
                last(way, t, 4).wait_recv()
                push(shard_of(way, 4, lax.rem(c + other, CORES)), (a, *CROSS[way])).start()

    @pl.when(c == 1)
    def _():
        message(partner, every, every).wait_send()
        over_chip(total_v, total_v).wait_send()

    @pl.when((col > 0) & (c == 1))
    def _():
        to_root().wait_send()
        answer(partner).wait_send()

    @pl.when(c * PLANE + col == PLANE)
    def _():
        ref = ins.at[0, pl.ds(0, 16 * PLANE)]
        pltpu.make_async_remote_copy(
            src_ref=ref, dst_ref=ref, send_sem=answer_send, recv_sem=answer_recv,
            device_id=partner, device_id_type=MESH,
        ).wait_send()

    @pl.when(c == 0)
    def _():
        over_chip(msg, both).wait_send()
        answer(partner).wait_recv()

    norm[...] = norm_f32[...].astype(jnp.bfloat16)

    def finish(core):
        def _():
            if EARLY[core]:
                ref = ins.at[pl.ds(0, 2), pl.ds(0, EARLY_AT[core][-1])] if EARLY_AT[core][-1] <= ROWS else ins.at[pl.ds(0, 4), pl.ds(0, EARLY_AT[core][-1] // 2)]
                hop(0, 0, ref, ref, early_send).wait_send()
            for a in range(3):
                own = sum(n for b, _, n in FIRST[core][EARLY[core] :] if b == a)
                ring_rows = 2 * (own + 2 * ROWS + (ROWS if core else 0))
                pushed = ROWS + 2 * (3 * ROWS + (ROWS if core else 0))
                crossing = sum(p[2] for way in (0, 1) for i, (_, p) in enumerate(BASE[way]) if crosses(way, i) and p[0] == a)
                come = ROWS + 2 * 3 * ROWS + (-crossing if core else 2 * ROWS)
                ref = rows_of(a, come)
                across(ref, a, push_recv.at[a]).wait_recv()
                ref = rows_of(a, ring_rows)
                hop(0, 0, ref, ref, ici_send.at[a]).wait_send()
                ref = rows_of(a, pushed)
                across(ref, a, push_recv.at[a]).wait_send()

        return _

    for core in range(CORES):
        pl.when(c == core)(finish(core))


def store_kernel(*refs):
    ins, outs, sem = refs[:7], refs[7:14], refs[14]
    for i, (src, dst) in enumerate(zip(ins, outs)):
        parts = PARTS if i < 3 else 1
        rows = src.shape[0] // parts
        for p in range(parts):
            window = pl.ds(p * rows, rows)
            pltpu.make_async_copy(src.at[window], dst.at[window], sem.at[i]).start()
    for i, (src, dst) in enumerate(zip(ins, outs)):
        pltpu.make_async_copy(src, dst, sem.at[i]).wait()


def store(arrays):
    return pl.pallas_call(
        store_kernel,
        name="store",
        out_shape=tuple(jax.ShapeDtypeStruct(a.shape, a.dtype) for a in arrays),
        in_specs=[pl.BlockSpec(memory_space=pltpu.VMEM)] * 7,
        out_specs=(pl.BlockSpec(memory_space=pltpu.HBM),) * 7,
        scratch_shapes=[pltpu.SemaphoreType.DMA((7,))],
        compiler_params=pltpu.CompilerParams(vmem_limit_bytes=16 * 2**20),
    )(*arrays)


def per_device(oq, tq, ok, tk, ov, tv, share, train, step):
    f32, bf16 = jnp.float32, jnp.bfloat16
    whole = jax.ShapeDtypeStruct((SHARDS * ROWS, 2 * LANES), bf16)
    scale = jax.ShapeDtypeStruct((1, 2 * LANES), f32)
    vmem = pl.BlockSpec(memory_space=pltpu.VMEM)
    dma = pltpu.SemaphoreType.DMA
    outs = pl.pallas_call(
        kernel,
        name="mix_and_gather",
        out_shape=(whole, whole, whole, scale, scale, scale, jax.ShapeDtypeStruct((32, LANES), bf16)),
        in_specs=[pl.BlockSpec(memory_space=pltpu.HBM)] * 9,
        out_specs=(vmem,) * 7,
        scratch_shapes=[
            pltpu.VMEM((6, ROWS, 2 * LANES), f32),
            pltpu.VMEM((1, ROWS), f32),
            pltpu.VMEM((2, 1, PIECE), f32),
            pltpu.VMEM((3, ROWS, 2 * LANES), f32),
            pltpu.VMEM((2, EARLY_ROWS, 2 * LANES), f32),
            pltpu.VMEM((8, LANES), f32),
            pltpu.VMEM((8, LANES), f32),
            pltpu.VMEM((8, LANES), f32),
            pltpu.VMEM((Z, 8, LANES), f32),
            pltpu.VMEM((SHARDS, LANES), f32),
            pltpu.VMEM((PLANE, SHARDS, LANES), f32),
            pltpu.VMEM((32, LANES), f32),
            dma((5,)),
            dma,
            dma,
            dma,
            dma,
            dma,
            dma,
            dma,
            dma,
            dma,
            dma((3,)),
            dma((2, STEPS + TAIL)),
            dma((3,)),
            dma((3,)),
            dma((2, 3)),
        ],
        compiler_params=pltpu.CompilerParams(
            collective_id=0, has_side_effects=True, vmem_limit_bytes=24 * 2**20
        ),
    )(*(pltpu.with_memory_space_constraint(a, pltpu.HBM) for a in (
        oq, tq, ok, tk, ov, tv, share.reshape(1, -1), train.reshape(1, -1), step.reshape(1, -1)
    )))
    q, k, v, scale_q, scale_k, scale_v, norm = store(outs)
    return q, k, v, scale_q.reshape(-1), scale_k.reshape(-1), scale_v.reshape(-1), norm.reshape(-1)


def solution(mesh):
    split = Mesh(mesh.devices.reshape(Z, CORES, PLANE_Y, PLANE_X), FSDP_COLS)
    block = P(FSDP, COLS)
    return jax.shard_map(
        per_device,
        mesh=split,
        in_specs=(block,) * 6 + (P(FSDP), P(FSDP_COLS), P(FSDP_COLS)),
        out_specs=(P(None, COLS),) * 3 + (P(COLS),) * 3 + (P(),),
        check_vma=False,
    )
```

```python
import functools
import math

import jax
import jax.numpy as jnp
from jax import lax
from jax.experimental import pallas as pl
from jax.experimental.pallas import tpu as pltpu
from jax.sharding import Mesh
from jax.sharding import PartitionSpec as P

FSDP = ("fsdp_0", "fsdp_1")
FSDP_COLS = ("fsdp_0", "fsdp_1", "cols_0", "cols_1")
COLS = ("cols_0", "cols_1")
MESH = pl.DeviceIdType.MESH

Z = 8
CORES = 2
SHARDS = Z * CORES
PLANE_Y = 4
PLANE_X = 4
PLANE = PLANE_Y * PLANE_X
ROWS = 256
HALF = 128
LANES = 128
PIECE = 16

WHOLE = [(a, 0, ROWS) for a in range(3)]
AHEAD = (ROWS, HALF)
FIRST = tuple(
    [(0, 0, n)] + [(0, n, ROWS - n)] * (n < ROWS) + [(1, 0, ROWS), (2, 0, ROWS)] for n in AHEAD
)
EARLY = (1, 1)
SPLIT = 128
CROSS = ((0, SPLIT), (SPLIT, ROWS - SPLIT))
LESS = 96
CROSS_TO_0 = ((0, LESS), (LESS, ROWS - LESS))
LAST_BEFORE_0 = (Z - 1, 1)
BASE = tuple(
    [(1, p) for p in range(max(len(f) for f in FIRST))]
    + [(2, p) for p in WHOLE]
    + [(3, p) for p in WHOLE[:2]]
    + [(3, p) for p in [(2, *CROSS_TO_0[way]), (2, *CROSS_TO_0[1 - way])] * (way == 1)
    + [(2, *CROSS[way]), (2, *CROSS[1 - way])] * (way == 0)]
    for way in (0, 1)
)
NEAR = sum(d == 1 for d, _ in BASE[0])
EARLY_AT = [[sum(n for _, _, n in f[:i]) for i in range(e + 1)] for f, e in zip(FIRST, EARLY)]
EARLY_ROWS = max(at[-1] for at in EARLY_AT)
STEPS = len(BASE[0])
LAST = [(a, other) for a in range(3) for other in (0, 1)]
TAIL = len(LAST)
ANSWER = 4
PASS = 7
LAG = 1
PARTS = 4


def kernel(
    oq, tq, ok, tk, ov, tv, share, train, step,
    out_q, out_k, out_v, scale_q, scale_k, scale_v, norm,
    ins, share_v, norm_in, mixed, landed, msg, both, total_v, sums, plane_out, plane_in, norm_f32,
    in_sem, chip_send, chip_recv, sum_send, sum_recv, plane_send, plane_recv, answer_send, answer_recv,
    early_send, ici_send, ici_recv, push_send, push_recv, cross_recv,
):
    z, c = lax.axis_index("fsdp_0"), lax.axis_index("fsdp_1")
    col = lax.axis_index("cols_0") * PLANE_X + lax.axis_index("cols_1")
    me = z * CORES + c
    outs = (out_q, out_k, out_v)

    ahead, behind = lax.rem(z + 1, Z), lax.rem(z + Z - 1, Z)
    partner = {"fsdp_1": 1 - c}

    def far_peers():
        for dz in (4, 5, 3, 6, 2, 7, 1):
            yield {"fsdp_0": lax.rem(z + dz, Z)}

    def plane_peers():
        for p in range(1, PLANE):
            yield {"cols_0": p // PLANE_X, "cols_1": p % PLANE_X}

    barrier = pltpu.get_barrier_semaphore()

    def greet(device):
        pl.semaphore_signal(barrier, inc=1, device_id=device, device_id_type=MESH)

    pltpu.make_async_copy(share, share_v, in_sem.at[3]).start()
    for i, src in enumerate((oq, tq, ok, tk, ov, tv)):
        pltpu.make_async_copy(src, ins.at[i], in_sem.at[i // 2]).start()
    for i, src in enumerate((train, step)):
        pltpu.make_async_copy(src, norm_in.at[i], in_sem.at[4]).start()

    @pl.when(c == 0)
    def _():
        for target in (ahead, behind):
            greet({"fsdp_0": target})

    @pl.when(c == 1)
    def _():
        for device in far_peers():
            greet(device)

    greet(partner)

    @pl.when(c * PLANE + col == PLANE)
    def _():
        for device in plane_peers():
            greet(device)

    def place(shard, piece):
        a, r, n = piece
        return outs[a].at[pl.ds(pl.multiple_of(shard * ROWS + r, math.gcd(ROWS, r, n)), n)]

    def shard_of(way, d, core):
        return lax.rem(z + (Z - d if way == 0 else d), Z) * CORES + core

    def hop(way, i, src, dst, send):
        target = ahead if way == 0 else behind
        return pltpu.make_async_remote_copy(
            src_ref=src, dst_ref=dst, send_sem=send, recv_sem=ici_recv.at[way, i],
            device_id={"fsdp_0": target}, device_id_type=MESH,
        )

    def early(way, i, core):
        a, r, n = FIRST[core][i]
        return hop(way, i, mixed.at[a, pl.ds(r, n)], landed.at[way, pl.ds(EARLY_AT[core][i], n)], early_send)

    def ring(way, i, shard):
        piece = BASE[way][i][1]
        ref = place(shard, piece)
        return hop(way, i, ref, ref, ici_send.at[piece[0]])

    def first(way, i, core, shard):
        piece = FIRST[core][i]
        ref = place(shard, piece)
        return hop(way, i, ref, ref, ici_send.at[piece[0]])

    def last(way, t, d, cross):
        a, other = LAST[t]
        core = lax.rem(c + other, CORES)
        ref = place(shard_of(way, d, core), (a, *cross[way]))
        return hop(way, t, ref, ref, ici_send.at[a])

    def by_target(way, d, act):
        special = LAST_BEFORE_0[way] if d == 3 else 0
        pl.when(z == special)(functools.partial(act, CROSS_TO_0))
        pl.when(z != special)(functools.partial(act, CROSS))

    def start_last(way, t):
        by_target(way, 3, lambda cross: last(way, t, 3, cross).start())

    def early_key():
        a, r, n = FIRST[0][1]
        return hop(1, 1, mixed.at[a], landed.at[1, pl.ds(EARLY_ROWS, n)], early_send)

    def across(ref, a, recv):
        return pltpu.make_async_remote_copy(
            src_ref=ref, dst_ref=ref, send_sem=push_send.at[a], recv_sem=recv,
            device_id=partner, device_id_type=MESH,
        )

    def push(shard, piece):
        return across(place(shard, piece), piece[0], push_recv.at[piece[0]])

    def rows_of(a, rows):
        return outs[a].at[pl.ds(0, rows)]

    msg[...] = jnp.zeros_like(msg)
    pltpu.make_async_copy(share, share_v, in_sem.at[3]).wait()
    shares = [
        jnp.broadcast_to(share_v[:, r * HALF : (r + 1) * HALF], (LANES, HALF)).T for r in range(2)
    ]
    for a in range(3):
        pair = ins.at[pl.ds(2 * a, 2)]
        pltpu.make_async_copy(pair, pair, in_sem.at[a]).wait()
        for j in range(2):
            lanes = pl.ds(j * LANES, LANES)
            total = jnp.zeros((1, LANES), jnp.float32)
            for r in range(2):
                rows = pl.ds(r * HALF, HALF)
                value = shares[r] * ins[2 * a, rows, lanes] + (1.0 - shares[r]) * ins[2 * a + 1, rows, lanes]
                mixed[a, rows, lanes] = value
                total = total + jnp.sum(value * value, axis=0, keepdims=True)
            msg[pl.ds(2 * a + j, 1), :] = total
    pltpu.make_async_copy(norm_in, norm_in, in_sem.at[4]).wait()
    piece = jnp.concatenate(
        [norm_in[0] + norm_in[1], jnp.zeros((1, LANES - PIECE), jnp.float32)], axis=1
    )
    piece = pltpu.roll(jnp.broadcast_to(piece, (8, LANES)), lax.rem(col, 8) * PIECE, 1)
    msg[pl.ds(6 + c, 1), :] = piece[:1]

    def over_chip(src, dst):
        return pltpu.make_async_remote_copy(
            src_ref=src, dst_ref=dst, send_sem=chip_send, recv_sem=chip_recv,
            device_id=partner, device_id_type=MESH,
        )

    def message(device, src, slot):
        return pltpu.make_async_remote_copy(
            src_ref=src, dst_ref=slot, send_sem=sum_send, recv_sem=sum_recv,
            device_id=device, device_id_type=MESH,
        )

    every = sums.at[pl.ds(0, Z - 1)]

    @pl.when(c == 0)
    def _():
        pl.semaphore_wait(barrier, 3)
        over_chip(msg, both).start()
        for i in range(EARLY[0]):
            for way in range(2):
                early(way, i, 0).start()
        pl.when(z == 1)(lambda: early_key().start())
        over_chip(total_v, total_v).wait_recv()

    @pl.when(c == 1)
    def _():
        pl.semaphore_wait(barrier, Z + (col + PLANE - 1) // PLANE)
        over_chip(msg, both).wait_recv()
        both[...] = both[...] + msg[...]
        for device in far_peers():
            message(device, both, sums.at[z]).start()
        for i in range(EARLY[1]):
            for way in range(2):
                early(way, i, 1).start()
        sums[pl.ds(z, 1)] = both[...][None]
        message(partner, every, every).wait_recv()
        total = sums[0]
        for s in range(1, Z):
            total = total + sums[s]
        total_v[...] = total
        over_chip(total_v, total_v).start()

    scale = jnp.sqrt(total_v[...])
    inverse = 1.0 / scale

    def put(shard, piece, read):
        a, r, n = piece
        rows = pl.ds(pl.multiple_of(shard * ROWS + r, math.gcd(ROWS, r, n)), n)
        for j in range(2):
            lanes = pl.ds(j * LANES, LANES)
            value = read(lanes) * inverse[2 * a + j : 2 * a + j + 1]
            outs[a][rows, lanes] = value.astype(jnp.bfloat16)

    def put_own(piece):
        a, r, n = piece
        put(me, piece, lambda lanes: mixed[a, pl.ds(r, n), lanes])

    def own_block(core):
        def _():
            late = list(range(EARLY[core], len(FIRST[core])))
            for k, i in enumerate(late + [None]):
                if i is not None:
                    put_own(FIRST[core][i])
                if k:
                    for way in range(2):
                        copy = first(way, late[k - 1], core, me)
                        if (core, way, late[k - 1]) == (0, 1, 1):
                            pl.when(z != 1)(copy.start)
                        else:
                            copy.start()
            for i in range(EARLY[core]):
                put_own(FIRST[core][i])

        return _

    for core in range(CORES):
        pl.when(c == core)(own_block(core))
    for piece in WHOLE:
        push(me, piece).start()

    for a, ref in enumerate((scale_q, scale_k, scale_v)):
        for j in range(2):
            ref[:, pl.ds(j * LANES, LANES)] = scale[2 * a + j : 2 * a + j + 1]

    def to_root():
        return pltpu.make_async_remote_copy(
            src_ref=plane_out, dst_ref=plane_in.at[col], send_sem=plane_send, recv_sem=plane_recv,
            device_id={"cols_0": 0, "cols_1": 0}, device_id_type=MESH,
        )

    def answer(device):
        return pltpu.make_async_remote_copy(
            src_ref=norm_f32, dst_ref=norm_f32, send_sem=answer_send, recv_sem=answer_recv,
            device_id=device, device_id_type=MESH,
        )

    @pl.when(c == 1)
    def _():
        for s in range(SHARDS):
            plane_out[pl.ds(s, 1), :] = sums[s // CORES, 6 + s % CORES : 7 + s % CORES, :]

    @pl.when((col > 0) & (c == 1))
    def _():
        to_root().start()

    def answer_all():
        plane_in[0] = plane_out[...]
        pieces = plane_in.at[pl.ds(1, PLANE - 1)]
        pltpu.make_async_remote_copy(
            src_ref=pieces, dst_ref=pieces, send_sem=plane_send, recv_sem=plane_recv,
            device_id={"cols_0": 0, "cols_1": 1}, device_id_type=MESH,
        ).wait_recv()
        for side in range(2):
            gathered = plane_in[8 * side]
            for k in range(1, 8):
                gathered = gathered + plane_in[8 * side + k]
            norm_f32[pl.ds(side, SHARDS, stride=2), :] = gathered
        for device in plane_peers():
            answer(device).start()
        answer(partner).start()

    def pass_on():
        answer({"cols_0": 0, "cols_1": 0}).wait_recv()
        answer(partner).start()

    def onward(way, i):
        d, piece = BASE[way][i]
        if d == 2:
            go_on(way, piece[0], 2)

    def go_on(way, a, d):
        for k, (far, piece) in enumerate(BASE[way]):
            if far == d + 1 and piece[0] == a:
                ring(way, k, shard_of(way, d, c)).start()

    def crosses(way, i):
        d, piece = BASE[way][i]
        return d == 3 and piece[1] <= CROSS[way][0] < piece[1] + piece[2]

    def from_partner(way, i):
        _, piece = BASE[way][i]
        a = piece[0]
        across(place(shard_of(way, 3, 1 - c), piece), a, cross_recv.at[way, a]).wait_recv()
        start_last(way, LAST.index((a, 1)))

    def near(way, i, core):
        piece = FIRST[core][i]
        a, r, n = piece
        shard = shard_of(way, 1, core)
        if i < EARLY[core]:
            early(way, i, core).wait_recv()
            put(shard, piece, lambda lanes: landed[way, pl.ds(EARLY_AT[core][i], n), lanes])
        elif (core, way, i) == (0, 1, 1):
            @pl.when(z == 0)
            def _():
                early_key().wait_recv()
                put(shard, piece, lambda lanes: landed[1, pl.ds(EARLY_ROWS, n), lanes])

            pl.when(z != 0)(lambda: first(way, i, core, shard).wait_recv())
        else:
            first(way, i, core, shard).wait_recv()
        if r + n == ROWS:
            go_on(way, a, 1)
        push(shard, piece).start()

    for i in range(STEPS + LAG):
        if i == ANSWER:
            pl.when(c * PLANE + col == PLANE)(answer_all)
        if i == PASS:
            pl.when((col > 0) & (c == 1))(pass_on)
        if i < STEPS:
            for way in range(2):
                d, piece = BASE[way][i]
                if d == 1:
                    for core in range(CORES):
                        if i < len(FIRST[core]):
                            pl.when(c == core)(functools.partial(near, way, i, core))
                    continue
                a = piece[0]
                shard = shard_of(way, d, c)
                ring(way, i, shard).wait_recv()
                onward(way, i)
                if crosses(way, i):
                    @pl.when(c == 1)
                    def _():
                        start_last(way, LAST.index((a, 0)))
                        push(shard, piece).start()

                    @pl.when(c == 0)
                    def _():
                        across(place(shard, piece), a, cross_recv.at[way, a]).start()
                else:
                    push(shard, piece).start()
        for way in range(2):
            if i >= LAG and crosses(way, i - LAG):
                pl.when(c == 1)(functools.partial(from_partner, way, i - LAG))

    @pl.when(c == 1)
    def _():
        for t, (a, other) in enumerate(LAST):
            for way in range(2):
                def take(cross):
                    last(way, t, 4, cross).wait_recv()
                    push(shard_of(way, 4, lax.rem(c + other, CORES)), (a, *cross[way])).start()

                by_target(way, 4, take)

    @pl.when(c == 1)
    def _():
        message(partner, every, every).wait_send()
        over_chip(total_v, total_v).wait_send()

    @pl.when((col > 0) & (c == 1))
    def _():
        to_root().wait_send()
        answer(partner).wait_send()

    @pl.when(c * PLANE + col == PLANE)
    def _():
        ref = ins.at[0, pl.ds(0, 16 * PLANE)]
        pltpu.make_async_remote_copy(
            src_ref=ref, dst_ref=ref, send_sem=answer_send, recv_sem=answer_recv,
            device_id=partner, device_id_type=MESH,
        ).wait_send()

    @pl.when(c == 0)
    def _():
        over_chip(msg, both).wait_send()
        answer(partner).wait_recv()

    norm[...] = norm_f32[...].astype(jnp.bfloat16)

    def sent_early(rows):
        ref = ins.at[pl.ds(0, rows // HALF), pl.ds(0, HALF)]
        hop(0, 0, ref, ref, early_send).wait_send()

    def sent_ring(a, rows):
        ref = rows_of(a, rows)
        hop(0, 0, ref, ref, ici_send.at[a]).wait_send()

    def finish(core):
        def _():
            early_rows = EARLY_AT[core][-1]
            if core == 0:
                pl.when(z == 1)(functools.partial(sent_early, 2 * early_rows + ROWS))
                pl.when(z != 1)(functools.partial(sent_early, 2 * early_rows))
            else:
                sent_early(2 * early_rows)
            for a in range(3):
                own = sum(n for b, _, n in FIRST[core][EARLY[core] :] if b == a)
                ring_rows = 2 * (own + 2 * ROWS + (ROWS if core else 0))
                fewer = 2 * (SPLIT - LESS)
                pushed = ROWS + 2 * (3 * ROWS + (ROWS if core else 0))
                crossing = sum(p[2] for way in (0, 1) for i, (_, p) in enumerate(BASE[way]) if crosses(way, i) and p[0] == a)
                come = ROWS + 2 * 3 * ROWS + (-crossing if core else 2 * ROWS)
                ref = rows_of(a, come)
                across(ref, a, push_recv.at[a]).wait_recv()
                if core == 1:
                    pl.when(z == Z - 1)(functools.partial(sent_ring, a, ring_rows - fewer))
                    pl.when(z == 1)(functools.partial(sent_ring, a, ring_rows + fewer))
                    pl.when((z > 1) & (z < Z - 1) | (z == 0))(functools.partial(sent_ring, a, ring_rows))
                elif a == 1:
                    pl.when(z == 1)(functools.partial(sent_ring, a, ring_rows - ROWS))
                    pl.when(z != 1)(functools.partial(sent_ring, a, ring_rows))
                else:
                    sent_ring(a, ring_rows)
                ref = rows_of(a, pushed)
                across(ref, a, push_recv.at[a]).wait_send()

        return _

    for core in range(CORES):
        pl.when(c == core)(finish(core))


def store_kernel(*refs):
    ins, outs, sem = refs[:7], refs[7:14], refs[14]
    for i, (src, dst) in enumerate(zip(ins, outs)):
        parts = PARTS if i < 3 else 1
        rows = src.shape[0] // parts
        for p in range(parts):
            window = pl.ds(p * rows, rows)
            pltpu.make_async_copy(src.at[window], dst.at[window], sem.at[i]).start()
    for i, (src, dst) in enumerate(zip(ins, outs)):
        pltpu.make_async_copy(src, dst, sem.at[i]).wait()


def store(arrays):
    return pl.pallas_call(
        store_kernel,
        name="store",
        out_shape=tuple(jax.ShapeDtypeStruct(a.shape, a.dtype) for a in arrays),
        in_specs=[pl.BlockSpec(memory_space=pltpu.VMEM)] * 7,
        out_specs=(pl.BlockSpec(memory_space=pltpu.HBM),) * 7,
        scratch_shapes=[pltpu.SemaphoreType.DMA((7,))],
        compiler_params=pltpu.CompilerParams(vmem_limit_bytes=16 * 2**20),
    )(*arrays)


def per_device(oq, tq, ok, tk, ov, tv, share, train, step):
    f32, bf16 = jnp.float32, jnp.bfloat16
    whole = jax.ShapeDtypeStruct((SHARDS * ROWS, 2 * LANES), bf16)
    scale = jax.ShapeDtypeStruct((1, 2 * LANES), f32)
    vmem = pl.BlockSpec(memory_space=pltpu.VMEM)
    dma = pltpu.SemaphoreType.DMA
    outs = pl.pallas_call(
        kernel,
        name="mix_and_gather",
        out_shape=(whole, whole, whole, scale, scale, scale, jax.ShapeDtypeStruct((32, LANES), bf16)),
        in_specs=[pl.BlockSpec(memory_space=pltpu.HBM)] * 9,
        out_specs=(vmem,) * 7,
        scratch_shapes=[
            pltpu.VMEM((6, ROWS, 2 * LANES), f32),
            pltpu.VMEM((1, ROWS), f32),
            pltpu.VMEM((2, 1, PIECE), f32),
            pltpu.VMEM((3, ROWS, 2 * LANES), f32),
            pltpu.VMEM((2, EARLY_ROWS + ROWS, 2 * LANES), f32),
            pltpu.VMEM((8, LANES), f32),
            pltpu.VMEM((8, LANES), f32),
            pltpu.VMEM((8, LANES), f32),
            pltpu.VMEM((Z, 8, LANES), f32),
            pltpu.VMEM((SHARDS, LANES), f32),
            pltpu.VMEM((PLANE, SHARDS, LANES), f32),
            pltpu.VMEM((32, LANES), f32),
            dma((5,)),
            dma,
            dma,
            dma,
            dma,
            dma,
            dma,
            dma,
            dma,
            dma,
            dma((3,)),
            dma((2, STEPS)),
            dma((3,)),
            dma((3,)),
            dma((2, 3)),
        ],
        compiler_params=pltpu.CompilerParams(
            collective_id=0, has_side_effects=True, vmem_limit_bytes=24 * 2**20
        ),
    )(*(pltpu.with_memory_space_constraint(a, pltpu.HBM) for a in (
        oq, tq, ok, tk, ov, tv, share.reshape(1, -1), train.reshape(1, -1), step.reshape(1, -1)
    )))
    q, k, v, scale_q, scale_k, scale_v, norm = store(outs)
    return q, k, v, scale_q.reshape(-1), scale_k.reshape(-1), scale_v.reshape(-1), norm.reshape(-1)


def solution(mesh):
    split = Mesh(mesh.devices.reshape(Z, CORES, PLANE_Y, PLANE_X), FSDP_COLS)
    block = P(FSDP, COLS)
    return jax.shard_map(
        per_device,
        mesh=split,
        in_specs=(block,) * 6 + (P(FSDP), P(FSDP_COLS), P(FSDP_COLS)),
        out_specs=(P(None, COLS),) * 3 + (P(COLS),) * 3 + (P(),),
        check_vma=False,
    )
```

```python
import functools
import math

import jax
import jax.numpy as jnp
from jax import lax
from jax.experimental import pallas as pl
from jax.experimental.pallas import tpu as pltpu
from jax.sharding import Mesh
from jax.sharding import PartitionSpec as P

FSDP = ("fsdp_0", "fsdp_1")
FSDP_COLS = ("fsdp_0", "fsdp_1", "cols_0", "cols_1")
COLS = ("cols_0", "cols_1")
MESH = pl.DeviceIdType.MESH

Z = 8
CORES = 2
SHARDS = Z * CORES
PLANE_Y = 4
PLANE_X = 4
PLANE = PLANE_Y * PLANE_X
ROWS = 256
HALF = 128
LANES = 128
PIECE = 16

WHOLE = [(a, 0, ROWS) for a in range(3)]
AHEAD = (ROWS, HALF)
FIRST = tuple(
    [(0, 0, n)] + [(0, n, ROWS - n)] * (n < ROWS) + [(1, 0, ROWS), (2, 0, ROWS)] for n in AHEAD
)
EARLY = (1, 1)
SPLIT = 120
CROSS = ((0, SPLIT), (SPLIT, ROWS - SPLIT))
LESS = 96
CROSS_TO_0 = ((0, LESS), (LESS, ROWS - LESS))
LAST_BEFORE_0 = (Z - 1, 1)
BASE = tuple(
    [(1, p) for p in range(max(len(f) for f in FIRST))]
    + [(2, p) for p in WHOLE]
    + [(3, p) for p in WHOLE[:2]]
    + [(3, p) for p in [(2, *CROSS_TO_0[way]), (2, *CROSS_TO_0[1 - way])] * (way == 1)
    + [(2, *CROSS[way]), (2, *CROSS[1 - way])] * (way == 0)]
    for way in (0, 1)
)
NEAR = sum(d == 1 for d, _ in BASE[0])
EARLY_AT = [[sum(n for _, _, n in f[:i]) for i in range(e + 1)] for f, e in zip(FIRST, EARLY)]
EARLY_ROWS = max(at[-1] for at in EARLY_AT)
STEPS = len(BASE[0])
LAST = [(a, other) for a in range(3) for other in (0, 1)]
TAIL = len(LAST)
ANSWER = 4
PASS = 7
LAG = 1
PARTS = 8


def kernel(
    oq, tq, ok, tk, ov, tv, share, train, step,
    out_q, out_k, out_v, scale_q, scale_k, scale_v, norm,
    ins, share_v, norm_in, mixed, landed, msg, both, total_v, sums, plane_out, plane_in, norm_f32,
    in_sem, chip_send, chip_recv, sum_send, sum_recv, plane_send, plane_recv, answer_send, answer_recv,
    early_send, ici_send, ici_recv, push_send, push_recv, cross_recv,
):
    z, c = lax.axis_index("fsdp_0"), lax.axis_index("fsdp_1")
    col = lax.axis_index("cols_0") * PLANE_X + lax.axis_index("cols_1")
    me = z * CORES + c
    outs = (out_q, out_k, out_v)

    ahead, behind = lax.rem(z + 1, Z), lax.rem(z + Z - 1, Z)
    partner = {"fsdp_1": 1 - c}

    def far_peers():
        for dz in (4, 5, 3, 6, 2, 7, 1):
            yield {"fsdp_0": lax.rem(z + dz, Z)}

    def plane_peers():
        for p in range(1, PLANE):
            yield {"cols_0": p // PLANE_X, "cols_1": p % PLANE_X}

    barrier = pltpu.get_barrier_semaphore()

    def greet(device):
        pl.semaphore_signal(barrier, inc=1, device_id=device, device_id_type=MESH)

    pltpu.make_async_copy(share, share_v, in_sem.at[3]).start()
    for i, src in enumerate((oq, tq, ok, tk, ov, tv)):
        pltpu.make_async_copy(src, ins.at[i], in_sem.at[i // 2]).start()
    for i, src in enumerate((train, step)):
        pltpu.make_async_copy(src, norm_in.at[i], in_sem.at[4]).start()

    @pl.when(c == 0)
    def _():
        for target in (ahead, behind):
            greet({"fsdp_0": target})

    @pl.when(c == 1)
    def _():
        for device in far_peers():
            greet(device)

    greet(partner)

    @pl.when(c * PLANE + col == PLANE)
    def _():
        for device in plane_peers():
            greet(device)

    def place(shard, piece):
        a, r, n = piece
        return outs[a].at[pl.ds(pl.multiple_of(shard * ROWS + r, math.gcd(ROWS, r, n)), n)]

    def shard_of(way, d, core):
        return lax.rem(z + (Z - d if way == 0 else d), Z) * CORES + core

    def hop(way, i, src, dst, send):
        target = ahead if way == 0 else behind
        return pltpu.make_async_remote_copy(
            src_ref=src, dst_ref=dst, send_sem=send, recv_sem=ici_recv.at[way, i],
            device_id={"fsdp_0": target}, device_id_type=MESH,
        )

    def early(way, i, core):
        a, r, n = FIRST[core][i]
        return hop(way, i, mixed.at[a, pl.ds(r, n)], landed.at[way, pl.ds(EARLY_AT[core][i], n)], early_send)

    def ring(way, i, shard):
        piece = BASE[way][i][1]
        ref = place(shard, piece)
        return hop(way, i, ref, ref, ici_send.at[piece[0]])

    def first(way, i, core, shard):
        piece = FIRST[core][i]
        ref = place(shard, piece)
        return hop(way, i, ref, ref, ici_send.at[piece[0]])

    def last(way, t, d, cross):
        a, other = LAST[t]
        core = lax.rem(c + other, CORES)
        ref = place(shard_of(way, d, core), (a, *cross[way]))
        return hop(way, t, ref, ref, ici_send.at[a])

    def by_target(way, d, act):
        special = LAST_BEFORE_0[way] if d == 3 else 0
        pl.when(z == special)(functools.partial(act, CROSS_TO_0))
        pl.when(z != special)(functools.partial(act, CROSS))

    def start_last(way, t):
        by_target(way, 3, lambda cross: last(way, t, 3, cross).start())

    def early_key():
        a, r, n = FIRST[0][1]
        return hop(1, 1, mixed.at[a], landed.at[1, pl.ds(EARLY_ROWS, n)], early_send)

    def across(ref, a, recv):
        return pltpu.make_async_remote_copy(
            src_ref=ref, dst_ref=ref, send_sem=push_send.at[a], recv_sem=recv,
            device_id=partner, device_id_type=MESH,
        )

    def push(shard, piece):
        return across(place(shard, piece), piece[0], push_recv.at[piece[0]])

    def rows_of(a, rows):
        return outs[a].at[pl.ds(0, rows)]

    msg[...] = jnp.zeros_like(msg)
    pltpu.make_async_copy(share, share_v, in_sem.at[3]).wait()
    shares = [
        jnp.broadcast_to(share_v[:, r * HALF : (r + 1) * HALF], (LANES, HALF)).T for r in range(2)
    ]
    for a in range(3):
        pair = ins.at[pl.ds(2 * a, 2)]
        pltpu.make_async_copy(pair, pair, in_sem.at[a]).wait()
        for j in range(2):
            lanes = pl.ds(j * LANES, LANES)
            total = jnp.zeros((1, LANES), jnp.float32)
            for r in range(2):
                rows = pl.ds(r * HALF, HALF)
                value = shares[r] * ins[2 * a, rows, lanes] + (1.0 - shares[r]) * ins[2 * a + 1, rows, lanes]
                mixed[a, rows, lanes] = value
                total = total + jnp.sum(value * value, axis=0, keepdims=True)
            msg[pl.ds(2 * a + j, 1), :] = total
    pltpu.make_async_copy(norm_in, norm_in, in_sem.at[4]).wait()
    piece = jnp.concatenate(
        [norm_in[0] + norm_in[1], jnp.zeros((1, LANES - PIECE), jnp.float32)], axis=1
    )
    piece = pltpu.roll(jnp.broadcast_to(piece, (8, LANES)), lax.rem(col, 8) * PIECE, 1)
    msg[pl.ds(6 + c, 1), :] = piece[:1]

    def over_chip(src, dst):
        return pltpu.make_async_remote_copy(
            src_ref=src, dst_ref=dst, send_sem=chip_send, recv_sem=chip_recv,
            device_id=partner, device_id_type=MESH,
        )

    def message(device, src, slot):
        return pltpu.make_async_remote_copy(
            src_ref=src, dst_ref=slot, send_sem=sum_send, recv_sem=sum_recv,
            device_id=device, device_id_type=MESH,
        )

    every = sums.at[pl.ds(0, Z - 1)]

    @pl.when(c == 0)
    def _():
        pl.semaphore_wait(barrier, 3)
        over_chip(msg, both).start()
        for i in range(EARLY[0]):
            for way in range(2):
                early(way, i, 0).start()
        pl.when(z == 1)(lambda: early_key().start())
        over_chip(total_v, total_v).wait_recv()

    @pl.when(c == 1)
    def _():
        pl.semaphore_wait(barrier, Z + (col + PLANE - 1) // PLANE)
        over_chip(msg, both).wait_recv()
        both[...] = both[...] + msg[...]
        for device in far_peers():
            message(device, both, sums.at[z]).start()
        for i in range(EARLY[1]):
            for way in range(2):
                early(way, i, 1).start()
        sums[pl.ds(z, 1)] = both[...][None]
        message(partner, every, every).wait_recv()
        total = sums[0]
        for s in range(1, Z):
            total = total + sums[s]
        total_v[...] = total
        over_chip(total_v, total_v).start()

    scale = jnp.sqrt(total_v[...])
    inverse = 1.0 / scale

    def put(shard, piece, read):
        a, r, n = piece
        rows = pl.ds(pl.multiple_of(shard * ROWS + r, math.gcd(ROWS, r, n)), n)
        for j in range(2):
            lanes = pl.ds(j * LANES, LANES)
            value = read(lanes) * inverse[2 * a + j : 2 * a + j + 1]
            outs[a][rows, lanes] = value.astype(jnp.bfloat16)

    def put_own(piece):
        a, r, n = piece
        put(me, piece, lambda lanes: mixed[a, pl.ds(r, n), lanes])

    def own_block(core):
        def _():
            late = list(range(EARLY[core], len(FIRST[core])))
            for k, i in enumerate(late + [None]):
                if i is not None:
                    put_own(FIRST[core][i])
                if k:
                    for way in range(2):
                        copy = first(way, late[k - 1], core, me)
                        if (core, way, late[k - 1]) == (0, 1, 1):
                            pl.when(z != 1)(copy.start)
                        else:
                            copy.start()
            for i in range(EARLY[core]):
                put_own(FIRST[core][i])

        return _

    for core in range(CORES):
        pl.when(c == core)(own_block(core))
    for piece in WHOLE:
        push(me, piece).start()

    for a, ref in enumerate((scale_q, scale_k, scale_v)):
        for j in range(2):
            ref[:, pl.ds(j * LANES, LANES)] = scale[2 * a + j : 2 * a + j + 1]

    def to_root():
        return pltpu.make_async_remote_copy(
            src_ref=plane_out, dst_ref=plane_in.at[col], send_sem=plane_send, recv_sem=plane_recv,
            device_id={"cols_0": 0, "cols_1": 0}, device_id_type=MESH,
        )

    def answer(device):
        return pltpu.make_async_remote_copy(
            src_ref=norm_f32, dst_ref=norm_f32, send_sem=answer_send, recv_sem=answer_recv,
            device_id=device, device_id_type=MESH,
        )

    @pl.when(c == 1)
    def _():
        for s in range(SHARDS):
            plane_out[pl.ds(s, 1), :] = sums[s // CORES, 6 + s % CORES : 7 + s % CORES, :]

    @pl.when((col > 0) & (c == 1))
    def _():
        to_root().start()

    def answer_all():
        plane_in[0] = plane_out[...]
        pieces = plane_in.at[pl.ds(1, PLANE - 1)]
        pltpu.make_async_remote_copy(
            src_ref=pieces, dst_ref=pieces, send_sem=plane_send, recv_sem=plane_recv,
            device_id={"cols_0": 0, "cols_1": 1}, device_id_type=MESH,
        ).wait_recv()
        for side in range(2):
            gathered = plane_in[8 * side]
            for k in range(1, 8):
                gathered = gathered + plane_in[8 * side + k]
            norm_f32[pl.ds(side, SHARDS, stride=2), :] = gathered
        for device in plane_peers():
            answer(device).start()
        answer(partner).start()

    def pass_on():
        answer({"cols_0": 0, "cols_1": 0}).wait_recv()
        answer(partner).start()

    def onward(way, i):
        d, piece = BASE[way][i]
        if d == 2:
            go_on(way, piece[0], 2)

    def go_on(way, a, d):
        for k, (far, piece) in enumerate(BASE[way]):
            if far == d + 1 and piece[0] == a:
                ring(way, k, shard_of(way, d, c)).start()

    def crosses(way, i):
        d, piece = BASE[way][i]
        return d == 3 and piece[1] <= CROSS[way][0] < piece[1] + piece[2]

    def from_partner(way, i):
        _, piece = BASE[way][i]
        a = piece[0]
        across(place(shard_of(way, 3, 1 - c), piece), a, cross_recv.at[way, a]).wait_recv()
        start_last(way, LAST.index((a, 1)))

    def near(way, i, core):
        piece = FIRST[core][i]
        a, r, n = piece
        shard = shard_of(way, 1, core)
        if i < EARLY[core]:
            early(way, i, core).wait_recv()
            put(shard, piece, lambda lanes: landed[way, pl.ds(EARLY_AT[core][i], n), lanes])
        elif (core, way, i) == (0, 1, 1):
            @pl.when(z == 0)
            def _():
                early_key().wait_recv()
                put(shard, piece, lambda lanes: landed[1, pl.ds(EARLY_ROWS, n), lanes])

            pl.when(z != 0)(lambda: first(way, i, core, shard).wait_recv())
        else:
            first(way, i, core, shard).wait_recv()
        if r + n == ROWS:
            go_on(way, a, 1)
        push(shard, piece).start()

    def arrived(way, i):
        d, piece = BASE[way][i]
        if d == 1:
            for core in range(CORES):
                if i < len(FIRST[core]):
                    pl.when(c == core)(functools.partial(near, way, i, core))
            return
        a = piece[0]
        shard = shard_of(way, d, c)
        ring(way, i, shard).wait_recv()
        onward(way, i)
        if crosses(way, i):
            @pl.when(c == 1)
            def _():
                start_last(way, LAST.index((a, 0)))
                push(shard, piece).start()

            @pl.when(c == 0)
            def _():
                across(place(shard, piece), a, cross_recv.at[way, a]).start()
        else:
            push(shard, piece).start()

    for i in range(STEPS + LAG):
        if i == ANSWER:
            pl.when(c * PLANE + col == PLANE)(answer_all)
        if i == PASS:
            pl.when((col > 0) & (c == 1))(pass_on)
        for way in range(2):
            if i < STEPS:
                arrived(way, i)
            if i >= LAG and crosses(way, i - LAG):
                pl.when(c == 1)(functools.partial(from_partner, way, i - LAG))

    @pl.when(c == 1)
    def _():
        for t, (a, other) in enumerate(LAST):
            for way in range(2):
                def take(cross):
                    last(way, t, 4, cross).wait_recv()
                    push(shard_of(way, 4, lax.rem(c + other, CORES)), (a, *cross[way])).start()

                by_target(way, 4, take)

    @pl.when(c == 1)
    def _():
        message(partner, every, every).wait_send()
        over_chip(total_v, total_v).wait_send()

    @pl.when((col > 0) & (c == 1))
    def _():
        to_root().wait_send()
        answer(partner).wait_send()

    @pl.when(c * PLANE + col == PLANE)
    def _():
        ref = ins.at[0, pl.ds(0, 16 * PLANE)]
        pltpu.make_async_remote_copy(
            src_ref=ref, dst_ref=ref, send_sem=answer_send, recv_sem=answer_recv,
            device_id=partner, device_id_type=MESH,
        ).wait_send()

    @pl.when(c == 0)
    def _():
        over_chip(msg, both).wait_send()
        answer(partner).wait_recv()

    norm[...] = norm_f32[...].astype(jnp.bfloat16)

    def sent_early(rows):
        ref = ins.at[pl.ds(0, rows // HALF), pl.ds(0, HALF)]
        hop(0, 0, ref, ref, early_send).wait_send()

    def sent_ring(a, rows):
        ref = rows_of(a, rows)
        hop(0, 0, ref, ref, ici_send.at[a]).wait_send()

    def finish(core):
        def _():
            early_rows = EARLY_AT[core][-1]
            if core == 0:
                pl.when(z == 1)(functools.partial(sent_early, 2 * early_rows + ROWS))
                pl.when(z != 1)(functools.partial(sent_early, 2 * early_rows))
            else:
                sent_early(2 * early_rows)
            for a in range(3):
                own = sum(n for b, _, n in FIRST[core][EARLY[core] :] if b == a)
                ring_rows = 2 * (own + 2 * ROWS + (ROWS if core else 0))
                fewer = 2 * (SPLIT - LESS)
                pushed = ROWS + 2 * (3 * ROWS + (ROWS if core else 0))
                crossing = sum(p[2] for way in (0, 1) for i, (_, p) in enumerate(BASE[way]) if crosses(way, i) and p[0] == a)
                come = ROWS + 2 * 3 * ROWS + (-crossing if core else 2 * ROWS)
                ref = rows_of(a, come)
                across(ref, a, push_recv.at[a]).wait_recv()
                if core == 1:
                    pl.when(z == Z - 1)(functools.partial(sent_ring, a, ring_rows - fewer))
                    pl.when(z == 1)(functools.partial(sent_ring, a, ring_rows + fewer))
                    pl.when((z > 1) & (z < Z - 1) | (z == 0))(functools.partial(sent_ring, a, ring_rows))
                elif a == 1:
                    pl.when(z == 1)(functools.partial(sent_ring, a, ring_rows - ROWS))
                    pl.when(z != 1)(functools.partial(sent_ring, a, ring_rows))
                else:
                    sent_ring(a, ring_rows)
                ref = rows_of(a, pushed)
                across(ref, a, push_recv.at[a]).wait_send()

        return _

    for core in range(CORES):
        pl.when(c == core)(finish(core))


def store_kernel(*refs):
    ins, outs, sem = refs[:7], refs[7:14], refs[14]
    for i, (src, dst) in enumerate(zip(ins, outs)):
        parts = PARTS if i < 3 else 1
        rows = src.shape[0] // parts
        for p in range(parts):
            window = pl.ds(p * rows, rows)
            pltpu.make_async_copy(src.at[window], dst.at[window], sem.at[i]).start()
    for i, (src, dst) in enumerate(zip(ins, outs)):
        pltpu.make_async_copy(src, dst, sem.at[i]).wait()


def store(arrays):
    return pl.pallas_call(
        store_kernel,
        name="store",
        out_shape=tuple(jax.ShapeDtypeStruct(a.shape, a.dtype) for a in arrays),
        in_specs=[pl.BlockSpec(memory_space=pltpu.VMEM)] * 7,
        out_specs=(pl.BlockSpec(memory_space=pltpu.HBM),) * 7,
        scratch_shapes=[pltpu.SemaphoreType.DMA((7,))],
        compiler_params=pltpu.CompilerParams(vmem_limit_bytes=16 * 2**20),
    )(*arrays)


def per_device(oq, tq, ok, tk, ov, tv, share, train, step):
    f32, bf16 = jnp.float32, jnp.bfloat16
    whole = jax.ShapeDtypeStruct((SHARDS * ROWS, 2 * LANES), bf16)
    scale = jax.ShapeDtypeStruct((1, 2 * LANES), f32)
    vmem = pl.BlockSpec(memory_space=pltpu.VMEM)
    dma = pltpu.SemaphoreType.DMA
    outs = pl.pallas_call(
        kernel,
        name="mix_and_gather",
        out_shape=(whole, whole, whole, scale, scale, scale, jax.ShapeDtypeStruct((32, LANES), bf16)),
        in_specs=[pl.BlockSpec(memory_space=pltpu.HBM)] * 9,
        out_specs=(vmem,) * 7,
        scratch_shapes=[
            pltpu.VMEM((6, ROWS, 2 * LANES), f32),
            pltpu.VMEM((1, ROWS), f32),
            pltpu.VMEM((2, 1, PIECE), f32),
            pltpu.VMEM((3, ROWS, 2 * LANES), f32),
            pltpu.VMEM((2, EARLY_ROWS + ROWS, 2 * LANES), f32),
            pltpu.VMEM((8, LANES), f32),
            pltpu.VMEM((8, LANES), f32),
            pltpu.VMEM((8, LANES), f32),
            pltpu.VMEM((Z, 8, LANES), f32),
            pltpu.VMEM((SHARDS, LANES), f32),
            pltpu.VMEM((PLANE, SHARDS, LANES), f32),
            pltpu.VMEM((32, LANES), f32),
            dma((5,)),
            dma,
            dma,
            dma,
            dma,
            dma,
            dma,
            dma,
            dma,
            dma,
            dma((3,)),
            dma((2, STEPS)),
            dma((3,)),
            dma((3,)),
            dma((2, 3)),
        ],
        compiler_params=pltpu.CompilerParams(
            collective_id=0, has_side_effects=True, vmem_limit_bytes=24 * 2**20
        ),
    )(*(pltpu.with_memory_space_constraint(a, pltpu.HBM) for a in (
        oq, tq, ok, tk, ov, tv, share.reshape(1, -1), train.reshape(1, -1), step.reshape(1, -1)
    )))
    q, k, v, scale_q, scale_k, scale_v, norm = store(outs)
    return q, k, v, scale_q.reshape(-1), scale_k.reshape(-1), scale_v.reshape(-1), norm.reshape(-1)


def solution(mesh):
    split = Mesh(mesh.devices.reshape(Z, CORES, PLANE_Y, PLANE_X), FSDP_COLS)
    block = P(FSDP, COLS)
    return jax.shard_map(
        per_device,
        mesh=split,
        in_specs=(block,) * 6 + (P(FSDP), P(FSDP_COLS), P(FSDP_COLS)),
        out_specs=(P(None, COLS),) * 3 + (P(COLS),) * 3 + (P(),),
        check_vma=False,
    )
```

```python
import functools
import math

import jax
import jax.numpy as jnp
from jax import lax
from jax.experimental import pallas as pl
from jax.experimental.pallas import tpu as pltpu
from jax.sharding import Mesh
from jax.sharding import PartitionSpec as P

FSDP = ("fsdp_0", "fsdp_1")
FSDP_COLS = ("fsdp_0", "fsdp_1", "cols_0", "cols_1")
COLS = ("cols_0", "cols_1")
MESH = pl.DeviceIdType.MESH

Z = 8
CORES = 2
SHARDS = Z * CORES
PLANE_Y = 4
PLANE_X = 4
PLANE = PLANE_Y * PLANE_X
ROWS = 256
HALF = 128
LANES = 128
PIECE = 16

WHOLE = [(a, 0, ROWS) for a in range(3)]
AHEAD = (ROWS, HALF)
FIRST = tuple(
    [(0, 0, n)] + [(0, n, ROWS - n)] * (n < ROWS) + [(1, 0, ROWS), (2, 0, ROWS)] for n in AHEAD
)
EARLY = (1, 1)
SPLIT = 120
CROSS = ((0, SPLIT), (SPLIT, ROWS - SPLIT))
LESS = 96
CROSS_TO_0 = ((0, LESS), (LESS, ROWS - LESS))
LAST_BEFORE_0 = (Z - 1, 1)
BASE = tuple(
    [(1, p) for p in range(max(len(f) for f in FIRST))]
    + [(2, p) for p in WHOLE]
    + [(3, p) for p in WHOLE[:2]]
    + [(3, p) for p in [(2, *CROSS_TO_0[way]), (2, *CROSS_TO_0[1 - way])] * (way == 1)
    + [(2, *CROSS[way]), (2, *CROSS[1 - way])] * (way == 0)]
    for way in (0, 1)
)
NEAR = sum(d == 1 for d, _ in BASE[0])
EARLY_AT = [[sum(n for _, _, n in f[:i]) for i in range(e + 1)] for f, e in zip(FIRST, EARLY)]
EARLY_ROWS = max(at[-1] for at in EARLY_AT)
STEPS = len(BASE[0])
LAST = [(a, other) for a in range(3) for other in (0, 1)]
TAIL = len(LAST)
ANSWER = 4
PASS = 7
LAG = 1
PARTS = 8


def kernel(
    oq, tq, ok, tk, ov, tv, share, train, step,
    out_q, out_k, out_v, scale_q, scale_k, scale_v, norm,
    ins, share_v, norm_in, mixed, landed, msg, both, total_v, sums, plane_out, plane_in, norm_f32,
    in_sem, chip_send, chip_recv, sum_send, sum_recv, plane_send, plane_recv, answer_send, answer_recv,
    early_send, ici_send, ici_recv, push_send, push_recv, cross_recv,
):
    z, c = lax.axis_index("fsdp_0"), lax.axis_index("fsdp_1")
    col = lax.axis_index("cols_0") * PLANE_X + lax.axis_index("cols_1")
    me = z * CORES + c
    outs = (out_q, out_k, out_v)

    ahead, behind = lax.rem(z + 1, Z), lax.rem(z + Z - 1, Z)
    partner = {"fsdp_1": 1 - c}

    def far_peers():
        for dz in (4, 5, 3, 6, 2, 7, 1):
            yield {"fsdp_0": lax.rem(z + dz, Z)}

    def plane_peers():
        for p in range(1, PLANE):
            yield {"cols_0": p // PLANE_X, "cols_1": p % PLANE_X}

    barrier = pltpu.get_barrier_semaphore()

    def greet(device):
        pl.semaphore_signal(barrier, inc=1, device_id=device, device_id_type=MESH)

    pltpu.make_async_copy(share, share_v, in_sem.at[3]).start()
    for i, src in enumerate((oq, tq, ok, tk, ov, tv)):
        pltpu.make_async_copy(src, ins.at[i], in_sem.at[i // 2]).start()
    for i, src in enumerate((train, step)):
        pltpu.make_async_copy(src, norm_in.at[i], in_sem.at[4]).start()

    @pl.when(c == 0)
    def _():
        for target in (ahead, behind):
            greet({"fsdp_0": target})

    @pl.when(c == 1)
    def _():
        for device in far_peers():
            greet(device)

    greet(partner)

    @pl.when(c * PLANE + col == PLANE)
    def _():
        for device in plane_peers():
            greet(device)

    def place(shard, piece):
        a, r, n = piece
        return outs[a].at[pl.ds(pl.multiple_of(shard * ROWS + r, math.gcd(ROWS, r, n)), n)]

    def shard_of(way, d, core):
        return lax.rem(z + (Z - d if way == 0 else d), Z) * CORES + core

    def hop(way, i, src, dst, send):
        target = ahead if way == 0 else behind
        return pltpu.make_async_remote_copy(
            src_ref=src, dst_ref=dst, send_sem=send, recv_sem=ici_recv.at[way, i],
            device_id={"fsdp_0": target}, device_id_type=MESH,
        )

    def early(way, i, core):
        a, r, n = FIRST[core][i]
        return hop(way, i, mixed.at[a, pl.ds(r, n)], landed.at[way, pl.ds(EARLY_AT[core][i], n)], early_send)

    def ring(way, i, shard):
        piece = BASE[way][i][1]
        ref = place(shard, piece)
        return hop(way, i, ref, ref, ici_send.at[piece[0]])

    def first(way, i, core, shard):
        piece = FIRST[core][i]
        ref = place(shard, piece)
        return hop(way, i, ref, ref, ici_send.at[piece[0]])

    def last(way, t, d, cross):
        a, other = LAST[t]
        core = lax.rem(c + other, CORES)
        ref = place(shard_of(way, d, core), (a, *cross[way]))
        return hop(way, t, ref, ref, ici_send.at[a])

    def by_target(way, d, act):
        special = LAST_BEFORE_0[way] if d == 3 else 0
        pl.when(z == special)(functools.partial(act, CROSS_TO_0))
        pl.when(z != special)(functools.partial(act, CROSS))

    def start_last(way, t):
        by_target(way, 3, lambda cross: last(way, t, 3, cross).start())

    def early_key():
        a, r, n = FIRST[0][1]
        return hop(1, 1, mixed.at[a], landed.at[1, pl.ds(EARLY_ROWS, n)], early_send)

    def across(ref, a, recv):
        return pltpu.make_async_remote_copy(
            src_ref=ref, dst_ref=ref, send_sem=push_send.at[a], recv_sem=recv,
            device_id=partner, device_id_type=MESH,
        )

    def push(shard, piece):
        return across(place(shard, piece), piece[0], push_recv.at[piece[0]])

    def rows_of(a, rows):
        return outs[a].at[pl.ds(0, rows)]

    msg[...] = jnp.zeros_like(msg)
    pltpu.make_async_copy(share, share_v, in_sem.at[3]).wait()
    shares = [
        jnp.broadcast_to(share_v[:, r * HALF : (r + 1) * HALF], (LANES, HALF)).T for r in range(2)
    ]
    for a in range(3):
        pair = ins.at[pl.ds(2 * a, 2)]
        pltpu.make_async_copy(pair, pair, in_sem.at[a]).wait()
        for j in range(2):
            lanes = pl.ds(j * LANES, LANES)
            total = jnp.zeros((1, LANES), jnp.float32)
            for r in range(2):
                rows = pl.ds(r * HALF, HALF)
                value = shares[r] * ins[2 * a, rows, lanes] + (1.0 - shares[r]) * ins[2 * a + 1, rows, lanes]
                mixed[a, rows, lanes] = value
                total = total + jnp.sum(value * value, axis=0, keepdims=True)
            msg[pl.ds(2 * a + j, 1), :] = total
        if a == 0:
            @pl.when(c == 0)
            def _():
                pl.semaphore_wait(barrier, 3)
                for i in range(EARLY[0]):
                    for way in range(2):
                        early(way, i, 0).start()

    pltpu.make_async_copy(norm_in, norm_in, in_sem.at[4]).wait()
    piece = jnp.concatenate(
        [norm_in[0] + norm_in[1], jnp.zeros((1, LANES - PIECE), jnp.float32)], axis=1
    )
    piece = pltpu.roll(jnp.broadcast_to(piece, (8, LANES)), lax.rem(col, 8) * PIECE, 1)
    msg[pl.ds(6 + c, 1), :] = piece[:1]

    def over_chip(src, dst):
        return pltpu.make_async_remote_copy(
            src_ref=src, dst_ref=dst, send_sem=chip_send, recv_sem=chip_recv,
            device_id=partner, device_id_type=MESH,
        )

    def message(device, src, slot):
        return pltpu.make_async_remote_copy(
            src_ref=src, dst_ref=slot, send_sem=sum_send, recv_sem=sum_recv,
            device_id=device, device_id_type=MESH,
        )

    every = sums.at[pl.ds(0, Z - 1)]

    @pl.when(c == 0)
    def _():
        over_chip(msg, both).start()
        pl.when(z == 1)(lambda: early_key().start())
        over_chip(total_v, total_v).wait_recv()

    @pl.when(c == 1)
    def _():
        pl.semaphore_wait(barrier, Z + (col + PLANE - 1) // PLANE)
        over_chip(msg, both).wait_recv()
        both[...] = both[...] + msg[...]
        for device in far_peers():
            message(device, both, sums.at[z]).start()
        for i in range(EARLY[1]):
            for way in range(2):
                early(way, i, 1).start()
        sums[pl.ds(z, 1)] = both[...][None]
        message(partner, every, every).wait_recv()
        total = sums[0]
        for s in range(1, Z):
            total = total + sums[s]
        total_v[...] = total
        over_chip(total_v, total_v).start()

    scale = jnp.sqrt(total_v[...])
    inverse = 1.0 / scale

    def put(shard, piece, read):
        a, r, n = piece
        rows = pl.ds(pl.multiple_of(shard * ROWS + r, math.gcd(ROWS, r, n)), n)
        for j in range(2):
            lanes = pl.ds(j * LANES, LANES)
            value = read(lanes) * inverse[2 * a + j : 2 * a + j + 1]
            outs[a][rows, lanes] = value.astype(jnp.bfloat16)

    def put_own(piece):
        a, r, n = piece
        put(me, piece, lambda lanes: mixed[a, pl.ds(r, n), lanes])

    def own_block(core):
        def _():
            late = list(range(EARLY[core], len(FIRST[core])))
            for k, i in enumerate(late + [None]):
                if i is not None:
                    put_own(FIRST[core][i])
                if k:
                    for way in range(2):
                        copy = first(way, late[k - 1], core, me)
                        if (core, way, late[k - 1]) == (0, 1, 1):
                            pl.when(z != 1)(copy.start)
                        else:
                            copy.start()
            for i in range(EARLY[core]):
                put_own(FIRST[core][i])

        return _

    for core in range(CORES):
        pl.when(c == core)(own_block(core))
    for piece in WHOLE:
        push(me, piece).start()

    for a, ref in enumerate((scale_q, scale_k, scale_v)):
        for j in range(2):
            ref[:, pl.ds(j * LANES, LANES)] = scale[2 * a + j : 2 * a + j + 1]

    def to_root():
        return pltpu.make_async_remote_copy(
            src_ref=plane_out, dst_ref=plane_in.at[col], send_sem=plane_send, recv_sem=plane_recv,
            device_id={"cols_0": 0, "cols_1": 0}, device_id_type=MESH,
        )

    def answer(device):
        return pltpu.make_async_remote_copy(
            src_ref=norm_f32, dst_ref=norm_f32, send_sem=answer_send, recv_sem=answer_recv,
            device_id=device, device_id_type=MESH,
        )

    @pl.when(c == 1)
    def _():
        for s in range(SHARDS):
            plane_out[pl.ds(s, 1), :] = sums[s // CORES, 6 + s % CORES : 7 + s % CORES, :]

    @pl.when((col > 0) & (c == 1))
    def _():
        to_root().start()

    def answer_all():
        plane_in[0] = plane_out[...]
        pieces = plane_in.at[pl.ds(1, PLANE - 1)]
        pltpu.make_async_remote_copy(
            src_ref=pieces, dst_ref=pieces, send_sem=plane_send, recv_sem=plane_recv,
            device_id={"cols_0": 0, "cols_1": 1}, device_id_type=MESH,
        ).wait_recv()
        for side in range(2):
            gathered = plane_in[8 * side]
            for k in range(1, 8):
                gathered = gathered + plane_in[8 * side + k]
            norm_f32[pl.ds(side, SHARDS, stride=2), :] = gathered
        for device in plane_peers():
            answer(device).start()
        answer(partner).start()

    def pass_on():
        answer({"cols_0": 0, "cols_1": 0}).wait_recv()
        answer(partner).start()

    def onward(way, i):
        d, piece = BASE[way][i]
        if d == 2:
            go_on(way, piece[0], 2)

    def go_on(way, a, d):
        for k, (far, piece) in enumerate(BASE[way]):
            if far == d + 1 and piece[0] == a:
                ring(way, k, shard_of(way, d, c)).start()

    def crosses(way, i):
        d, piece = BASE[way][i]
        return d == 3 and piece[1] <= CROSS[way][0] < piece[1] + piece[2]

    def from_partner(way, i):
        _, piece = BASE[way][i]
        a = piece[0]
        across(place(shard_of(way, 3, 1 - c), piece), a, cross_recv.at[way, a]).wait_recv()
        start_last(way, LAST.index((a, 1)))

    def near(way, i, core):
        piece = FIRST[core][i]
        a, r, n = piece
        shard = shard_of(way, 1, core)
        if i < EARLY[core]:
            early(way, i, core).wait_recv()
            put(shard, piece, lambda lanes: landed[way, pl.ds(EARLY_AT[core][i], n), lanes])
        elif (core, way, i) == (0, 1, 1):
            @pl.when(z == 0)
            def _():
                early_key().wait_recv()
                put(shard, piece, lambda lanes: landed[1, pl.ds(EARLY_ROWS, n), lanes])

            pl.when(z != 0)(lambda: first(way, i, core, shard).wait_recv())
        else:
            first(way, i, core, shard).wait_recv()
        if r + n == ROWS:
            go_on(way, a, 1)
        push(shard, piece).start()

    def arrived(way, i):
        d, piece = BASE[way][i]
        if d == 1:
            for core in range(CORES):
                if i < len(FIRST[core]):
                    pl.when(c == core)(functools.partial(near, way, i, core))
            return
        a = piece[0]
        shard = shard_of(way, d, c)
        ring(way, i, shard).wait_recv()
        onward(way, i)
        if crosses(way, i):
            @pl.when(c == 1)
            def _():
                start_last(way, LAST.index((a, 0)))
                push(shard, piece).start()

            @pl.when(c == 0)
            def _():
                across(place(shard, piece), a, cross_recv.at[way, a]).start()
        else:
            push(shard, piece).start()

    for i in range(STEPS + LAG):
        if i == ANSWER:
            pl.when(c * PLANE + col == PLANE)(answer_all)
        if i == PASS:
            pl.when((col > 0) & (c == 1))(pass_on)
        for way in range(2):
            if i < STEPS:
                arrived(way, i)
            if i >= LAG and crosses(way, i - LAG):
                pl.when(c == 1)(functools.partial(from_partner, way, i - LAG))

    @pl.when(c == 1)
    def _():
        for t, (a, other) in enumerate(LAST):
            for way in range(2):
                def take(cross):
                    last(way, t, 4, cross).wait_recv()
                    push(shard_of(way, 4, lax.rem(c + other, CORES)), (a, *cross[way])).start()

                by_target(way, 4, take)

    @pl.when(c == 1)
    def _():
        message(partner, every, every).wait_send()
        over_chip(total_v, total_v).wait_send()

    @pl.when((col > 0) & (c == 1))
    def _():
        to_root().wait_send()
        answer(partner).wait_send()

    @pl.when(c * PLANE + col == PLANE)
    def _():
        ref = ins.at[0, pl.ds(0, 16 * PLANE)]
        pltpu.make_async_remote_copy(
            src_ref=ref, dst_ref=ref, send_sem=answer_send, recv_sem=answer_recv,
            device_id=partner, device_id_type=MESH,
        ).wait_send()

    @pl.when(c == 0)
    def _():
        over_chip(msg, both).wait_send()
        answer(partner).wait_recv()

    norm[...] = norm_f32[...].astype(jnp.bfloat16)

    def sent_early(rows):
        ref = ins.at[pl.ds(0, rows // HALF), pl.ds(0, HALF)]
        hop(0, 0, ref, ref, early_send).wait_send()

    def sent_ring(a, rows):
        ref = rows_of(a, rows)
        hop(0, 0, ref, ref, ici_send.at[a]).wait_send()

    def finish(core):
        def _():
            early_rows = EARLY_AT[core][-1]
            if core == 0:
                pl.when(z == 1)(functools.partial(sent_early, 2 * early_rows + ROWS))
                pl.when(z != 1)(functools.partial(sent_early, 2 * early_rows))
            else:
                sent_early(2 * early_rows)
            for a in range(3):
                own = sum(n for b, _, n in FIRST[core][EARLY[core] :] if b == a)
                ring_rows = 2 * (own + 2 * ROWS + (ROWS if core else 0))
                fewer = 2 * (SPLIT - LESS)
                pushed = ROWS + 2 * (3 * ROWS + (ROWS if core else 0))
                crossing = sum(p[2] for way in (0, 1) for i, (_, p) in enumerate(BASE[way]) if crosses(way, i) and p[0] == a)
                come = ROWS + 2 * 3 * ROWS + (-crossing if core else 2 * ROWS)
                ref = rows_of(a, come)
                across(ref, a, push_recv.at[a]).wait_recv()
                if core == 1:
                    pl.when(z == Z - 1)(functools.partial(sent_ring, a, ring_rows - fewer))
                    pl.when(z == 1)(functools.partial(sent_ring, a, ring_rows + fewer))
                    pl.when((z > 1) & (z < Z - 1) | (z == 0))(functools.partial(sent_ring, a, ring_rows))
                elif a == 1:
                    pl.when(z == 1)(functools.partial(sent_ring, a, ring_rows - ROWS))
                    pl.when(z != 1)(functools.partial(sent_ring, a, ring_rows))
                else:
                    sent_ring(a, ring_rows)
                ref = rows_of(a, pushed)
                across(ref, a, push_recv.at[a]).wait_send()

        return _

    for core in range(CORES):
        pl.when(c == core)(finish(core))


def store_kernel(*refs):
    ins, outs, sem = refs[:7], refs[7:14], refs[14]
    for i, (src, dst) in enumerate(zip(ins, outs)):
        parts = PARTS if i < 3 else 1
        rows = src.shape[0] // parts
        for p in range(parts):
            window = pl.ds(p * rows, rows)
            pltpu.make_async_copy(src.at[window], dst.at[window], sem.at[i]).start()
    for i, (src, dst) in enumerate(zip(ins, outs)):
        pltpu.make_async_copy(src, dst, sem.at[i]).wait()


def store(arrays):
    return pl.pallas_call(
        store_kernel,
        name="store",
        out_shape=tuple(jax.ShapeDtypeStruct(a.shape, a.dtype) for a in arrays),
        in_specs=[pl.BlockSpec(memory_space=pltpu.VMEM)] * 7,
        out_specs=(pl.BlockSpec(memory_space=pltpu.HBM),) * 7,
        scratch_shapes=[pltpu.SemaphoreType.DMA((7,))],
        compiler_params=pltpu.CompilerParams(vmem_limit_bytes=16 * 2**20),
    )(*arrays)


def per_device(oq, tq, ok, tk, ov, tv, share, train, step):
    f32, bf16 = jnp.float32, jnp.bfloat16
    whole = jax.ShapeDtypeStruct((SHARDS * ROWS, 2 * LANES), bf16)
    scale = jax.ShapeDtypeStruct((1, 2 * LANES), f32)
    vmem = pl.BlockSpec(memory_space=pltpu.VMEM)
    dma = pltpu.SemaphoreType.DMA
    outs = pl.pallas_call(
        kernel,
        name="mix_and_gather",
        out_shape=(whole, whole, whole, scale, scale, scale, jax.ShapeDtypeStruct((32, LANES), bf16)),
        in_specs=[pl.BlockSpec(memory_space=pltpu.HBM)] * 9,
        out_specs=(vmem,) * 7,
        scratch_shapes=[
            pltpu.VMEM((6, ROWS, 2 * LANES), f32),
            pltpu.VMEM((1, ROWS), f32),
            pltpu.VMEM((2, 1, PIECE), f32),
            pltpu.VMEM((3, ROWS, 2 * LANES), f32),
            pltpu.VMEM((2, EARLY_ROWS + ROWS, 2 * LANES), f32),
            pltpu.VMEM((8, LANES), f32),
            pltpu.VMEM((8, LANES), f32),
            pltpu.VMEM((8, LANES), f32),
            pltpu.VMEM((Z, 8, LANES), f32),
            pltpu.VMEM((SHARDS, LANES), f32),
            pltpu.VMEM((PLANE, SHARDS, LANES), f32),
            pltpu.VMEM((32, LANES), f32),
            dma((5,)),
            dma,
            dma,
            dma,
            dma,
            dma,
            dma,
            dma,
            dma,
            dma,
            dma((3,)),
            dma((2, STEPS)),
            dma((3,)),
            dma((3,)),
            dma((2, 3)),
        ],
        compiler_params=pltpu.CompilerParams(
            collective_id=0, has_side_effects=True, vmem_limit_bytes=24 * 2**20
        ),
    )(*(pltpu.with_memory_space_constraint(a, pltpu.HBM) for a in (
        oq, tq, ok, tk, ov, tv, share.reshape(1, -1), train.reshape(1, -1), step.reshape(1, -1)
    )))
    q, k, v, scale_q, scale_k, scale_v, norm = store(outs)
    return q, k, v, scale_q.reshape(-1), scale_k.reshape(-1), scale_v.reshape(-1), norm.reshape(-1)


def solution(mesh):
    split = Mesh(mesh.devices.reshape(Z, CORES, PLANE_Y, PLANE_X), FSDP_COLS)
    block = P(FSDP, COLS)
    return jax.shard_map(
        per_device,
        mesh=split,
        in_specs=(block,) * 6 + (P(FSDP), P(FSDP_COLS), P(FSDP_COLS)),
        out_specs=(P(None, COLS),) * 3 + (P(COLS),) * 3 + (P(),),
        check_vma=False,
    )
```

```python
import functools
import math

import jax
import jax.numpy as jnp
from jax import lax
from jax.experimental import pallas as pl
from jax.experimental.pallas import tpu as pltpu
from jax.sharding import Mesh
from jax.sharding import PartitionSpec as P

FSDP = ("fsdp_0", "fsdp_1")
FSDP_COLS = ("fsdp_0", "fsdp_1", "cols_0", "cols_1")
COLS = ("cols_0", "cols_1")
MESH = pl.DeviceIdType.MESH

Z = 8
CORES = 2
SHARDS = Z * CORES
PLANE_Y = 4
PLANE_X = 4
PLANE = PLANE_Y * PLANE_X
ROWS = 256
HALF = 128
LANES = 128
PIECE = 16

WHOLE = [(a, 0, ROWS) for a in range(3)]
FIRST = (
    [(0, 0, ROWS), (1, 0, ROWS), (2, 0, ROWS)],
    [(0, 0, 32), (0, 32, 96), (0, HALF, HALF), (1, 0, ROWS), (2, 0, ROWS)],
)
EARLY = (1, 2)
SPLIT = 120
CROSS = ((0, SPLIT), (SPLIT, ROWS - SPLIT))
LESS = 96
CROSS_TO_0 = ((0, LESS), (LESS, ROWS - LESS))
LAST_BEFORE_0 = (Z - 1, 1)
BASE = tuple(
    [(1, p) for p in range(max(len(f) for f in FIRST))]
    + [(2, p) for p in WHOLE]
    + [(3, p) for p in WHOLE[:2]]
    + [(3, p) for p in [(2, *CROSS_TO_0[way]), (2, *CROSS_TO_0[1 - way])] * (way == 1)
    + [(2, *CROSS[way]), (2, *CROSS[1 - way])] * (way == 0)]
    for way in (0, 1)
)
NEAR = sum(d == 1 for d, _ in BASE[0])
EARLY_AT = [[sum(n for _, _, n in f[:i]) for i in range(e + 1)] for f, e in zip(FIRST, EARLY)]
EARLY_ROWS = max(at[-1] for at in EARLY_AT)
STEPS = len(BASE[0])
LAST = [(a, other) for a in range(3) for other in (0, 1)]
TAIL = len(LAST)
ANSWER = 4
PASS = 7
LAG = 1
PARTS = 8


def kernel(
    oq, tq, ok, tk, ov, tv, share, train, step,
    out_q, out_k, out_v, scale_q, scale_k, scale_v, norm,
    ins, share_v, norm_in, mixed, landed, msg, both, total_v, sums, plane_out, plane_in, norm_f32,
    in_sem, chip_send, chip_recv, sum_send, sum_recv, plane_send, plane_recv, answer_send, answer_recv,
    early_send, ici_send, ici_recv, push_send, push_recv, cross_recv,
):
    z, c = lax.axis_index("fsdp_0"), lax.axis_index("fsdp_1")
    col = lax.axis_index("cols_0") * PLANE_X + lax.axis_index("cols_1")
    me = z * CORES + c
    outs = (out_q, out_k, out_v)

    ahead, behind = lax.rem(z + 1, Z), lax.rem(z + Z - 1, Z)
    partner = {"fsdp_1": 1 - c}

    def far_peers():
        for dz in (4, 5, 3, 6, 2, 7, 1):
            yield {"fsdp_0": lax.rem(z + dz, Z)}

    def plane_peers():
        for p in range(1, PLANE):
            yield {"cols_0": p // PLANE_X, "cols_1": p % PLANE_X}

    barrier = pltpu.get_barrier_semaphore()

    def greet(device):
        pl.semaphore_signal(barrier, inc=1, device_id=device, device_id_type=MESH)

    pltpu.make_async_copy(share, share_v, in_sem.at[3]).start()
    for i, src in enumerate((oq, tq, ok, tk, ov, tv)):
        pltpu.make_async_copy(src, ins.at[i], in_sem.at[i // 2]).start()
    for i, src in enumerate((train, step)):
        pltpu.make_async_copy(src, norm_in.at[i], in_sem.at[4]).start()

    @pl.when(c == 0)
    def _():
        for target in (ahead, behind):
            greet({"fsdp_0": target})

    @pl.when(c == 1)
    def _():
        for device in far_peers():
            greet(device)

    greet(partner)

    @pl.when(c * PLANE + col == PLANE)
    def _():
        for device in plane_peers():
            greet(device)

    def place(shard, piece):
        a, r, n = piece
        return outs[a].at[pl.ds(pl.multiple_of(shard * ROWS + r, math.gcd(ROWS, r, n)), n)]

    def shard_of(way, d, core):
        return lax.rem(z + (Z - d if way == 0 else d), Z) * CORES + core

    def hop(way, i, src, dst, send):
        target = ahead if way == 0 else behind
        return pltpu.make_async_remote_copy(
            src_ref=src, dst_ref=dst, send_sem=send, recv_sem=ici_recv.at[way, i],
            device_id={"fsdp_0": target}, device_id_type=MESH,
        )

    def early(way, i, core):
        a, r, n = FIRST[core][i]
        return hop(way, i, mixed.at[a, pl.ds(r, n)], landed.at[way, pl.ds(EARLY_AT[core][i], n)], early_send)

    def ring(way, i, shard):
        piece = BASE[way][i][1]
        ref = place(shard, piece)
        return hop(way, i, ref, ref, ici_send.at[piece[0]])

    def first(way, i, core, shard):
        piece = FIRST[core][i]
        ref = place(shard, piece)
        return hop(way, i, ref, ref, ici_send.at[piece[0]])

    def last(way, t, d, cross):
        a, other = LAST[t]
        core = lax.rem(c + other, CORES)
        ref = place(shard_of(way, d, core), (a, *cross[way]))
        return hop(way, t, ref, ref, ici_send.at[a])

    def by_target(way, d, act):
        special = LAST_BEFORE_0[way] if d == 3 else 0
        pl.when(z == special)(functools.partial(act, CROSS_TO_0))
        pl.when(z != special)(functools.partial(act, CROSS))

    def start_last(way, t):
        by_target(way, 3, lambda cross: last(way, t, 3, cross).start())

    def early_key():
        a, r, n = FIRST[0][1]
        return hop(1, 1, mixed.at[a], landed.at[1, pl.ds(EARLY_ROWS, n)], early_send)

    def across(ref, a, recv):
        return pltpu.make_async_remote_copy(
            src_ref=ref, dst_ref=ref, send_sem=push_send.at[a], recv_sem=recv,
            device_id=partner, device_id_type=MESH,
        )

    def push(shard, piece):
        return across(place(shard, piece), piece[0], push_recv.at[piece[0]])

    def rows_of(a, rows):
        return outs[a].at[pl.ds(0, rows)]

    msg[...] = jnp.zeros_like(msg)
    pltpu.make_async_copy(share, share_v, in_sem.at[3]).wait()
    shares = [
        jnp.broadcast_to(share_v[:, r * HALF : (r + 1) * HALF], (LANES, HALF)).T for r in range(2)
    ]
    for a in range(3):
        pair = ins.at[pl.ds(2 * a, 2)]
        pltpu.make_async_copy(pair, pair, in_sem.at[a]).wait()
        for j in range(2):
            lanes = pl.ds(j * LANES, LANES)
            total = jnp.zeros((1, LANES), jnp.float32)
            for r in range(2):
                rows = pl.ds(r * HALF, HALF)
                value = shares[r] * ins[2 * a, rows, lanes] + (1.0 - shares[r]) * ins[2 * a + 1, rows, lanes]
                mixed[a, rows, lanes] = value
                total = total + jnp.sum(value * value, axis=0, keepdims=True)
            msg[pl.ds(2 * a + j, 1), :] = total
    pltpu.make_async_copy(norm_in, norm_in, in_sem.at[4]).wait()
    piece = jnp.concatenate(
        [norm_in[0] + norm_in[1], jnp.zeros((1, LANES - PIECE), jnp.float32)], axis=1
    )
    piece = pltpu.roll(jnp.broadcast_to(piece, (8, LANES)), lax.rem(col, 8) * PIECE, 1)
    msg[pl.ds(6 + c, 1), :] = piece[:1]

    def over_chip(src, dst):
        return pltpu.make_async_remote_copy(
            src_ref=src, dst_ref=dst, send_sem=chip_send, recv_sem=chip_recv,
            device_id=partner, device_id_type=MESH,
        )

    def message(device, src, slot):
        return pltpu.make_async_remote_copy(
            src_ref=src, dst_ref=slot, send_sem=sum_send, recv_sem=sum_recv,
            device_id=device, device_id_type=MESH,
        )

    every = sums.at[pl.ds(0, Z - 1)]

    @pl.when(c == 0)
    def _():
        pl.semaphore_wait(barrier, 3)
        over_chip(msg, both).start()
        for i in range(EARLY[0]):
            for way in range(2):
                early(way, i, 0).start()
        pl.when(z == 1)(lambda: early_key().start())
        over_chip(total_v, total_v).wait_recv()

    @pl.when(c == 1)
    def _():
        pl.semaphore_wait(barrier, Z + (col + PLANE - 1) // PLANE)
        def first_rows():
            for way in range(2):
                early(way, 0, 1).start()

        pl.when(z >= Z // 2)(first_rows)
        over_chip(msg, both).wait_recv()
        both[...] = both[...] + msg[...]
        for device in far_peers():
            message(device, both, sums.at[z]).start()
        pl.when(z < Z // 2)(first_rows)
        for i in range(1, EARLY[1]):
            for way in range(2):
                early(way, i, 1).start()
        sums[pl.ds(z, 1)] = both[...][None]
        message(partner, every, every).wait_recv()
        total = sums[0]
        for s in range(1, Z):
            total = total + sums[s]
        total_v[...] = total
        over_chip(total_v, total_v).start()

    scale = jnp.sqrt(total_v[...])
    inverse = 1.0 / scale

    def put(shard, piece, read):
        a, r, n = piece
        rows = pl.ds(pl.multiple_of(shard * ROWS + r, math.gcd(ROWS, r, n)), n)
        for j in range(2):
            lanes = pl.ds(j * LANES, LANES)
            value = read(lanes) * inverse[2 * a + j : 2 * a + j + 1]
            outs[a][rows, lanes] = value.astype(jnp.bfloat16)

    def put_own(piece):
        a, r, n = piece
        put(me, piece, lambda lanes: mixed[a, pl.ds(r, n), lanes])

    def own_block(core):
        def _():
            late = list(range(EARLY[core], len(FIRST[core])))
            for k, i in enumerate(late + [None]):
                if i is not None:
                    put_own(FIRST[core][i])
                if k:
                    for way in range(2):
                        copy = first(way, late[k - 1], core, me)
                        if (core, way, late[k - 1]) == (0, 1, 1):
                            pl.when(z != 1)(copy.start)
                        else:
                            copy.start()
            for i in range(EARLY[core]):
                put_own(FIRST[core][i])

        return _

    for core in range(CORES):
        pl.when(c == core)(own_block(core))
    for piece in WHOLE:
        push(me, piece).start()

    for a, ref in enumerate((scale_q, scale_k, scale_v)):
        for j in range(2):
            ref[:, pl.ds(j * LANES, LANES)] = scale[2 * a + j : 2 * a + j + 1]

    def to_root():
        return pltpu.make_async_remote_copy(
            src_ref=plane_out, dst_ref=plane_in.at[col], send_sem=plane_send, recv_sem=plane_recv,
            device_id={"cols_0": 0, "cols_1": 0}, device_id_type=MESH,
        )

    def answer(device):
        return pltpu.make_async_remote_copy(
            src_ref=norm_f32, dst_ref=norm_f32, send_sem=answer_send, recv_sem=answer_recv,
            device_id=device, device_id_type=MESH,
        )

    @pl.when(c == 1)
    def _():
        for s in range(SHARDS):
            plane_out[pl.ds(s, 1), :] = sums[s // CORES, 6 + s % CORES : 7 + s % CORES, :]

    @pl.when((col > 0) & (c == 1))
    def _():
        to_root().start()

    def answer_all():
        plane_in[0] = plane_out[...]
        pieces = plane_in.at[pl.ds(1, PLANE - 1)]
        pltpu.make_async_remote_copy(
            src_ref=pieces, dst_ref=pieces, send_sem=plane_send, recv_sem=plane_recv,
            device_id={"cols_0": 0, "cols_1": 1}, device_id_type=MESH,
        ).wait_recv()
        for side in range(2):
            gathered = plane_in[8 * side]
            for k in range(1, 8):
                gathered = gathered + plane_in[8 * side + k]
            norm_f32[pl.ds(side, SHARDS, stride=2), :] = gathered
        for device in plane_peers():
            answer(device).start()
        answer(partner).start()

    def pass_on():
        answer({"cols_0": 0, "cols_1": 0}).wait_recv()
        answer(partner).start()

    def onward(way, i):
        d, piece = BASE[way][i]
        if d == 2:
            go_on(way, piece[0], 2)

    def go_on(way, a, d):
        for k, (far, piece) in enumerate(BASE[way]):
            if far == d + 1 and piece[0] == a:
                ring(way, k, shard_of(way, d, c)).start()

    def crosses(way, i):
        d, piece = BASE[way][i]
        return d == 3 and piece[1] <= CROSS[way][0] < piece[1] + piece[2]

    def from_partner(way, i):
        _, piece = BASE[way][i]
        a = piece[0]
        across(place(shard_of(way, 3, 1 - c), piece), a, cross_recv.at[way, a]).wait_recv()
        start_last(way, LAST.index((a, 1)))

    def near(way, i, core):
        piece = FIRST[core][i]
        a, r, n = piece
        shard = shard_of(way, 1, core)
        if i < EARLY[core]:
            early(way, i, core).wait_recv()
            put(shard, piece, lambda lanes: landed[way, pl.ds(EARLY_AT[core][i], n), lanes])
        elif (core, way, i) == (0, 1, 1):
            @pl.when(z == 0)
            def _():
                early_key().wait_recv()
                put(shard, piece, lambda lanes: landed[1, pl.ds(EARLY_ROWS, n), lanes])

            pl.when(z != 0)(lambda: first(way, i, core, shard).wait_recv())
        else:
            first(way, i, core, shard).wait_recv()
        if r + n == ROWS:
            go_on(way, a, 1)
        push(shard, piece).start()

    def arrived(way, i):
        d, piece = BASE[way][i]
        if d == 1:
            for core in range(CORES):
                if i < len(FIRST[core]):
                    pl.when(c == core)(functools.partial(near, way, i, core))
            return
        a = piece[0]
        shard = shard_of(way, d, c)
        ring(way, i, shard).wait_recv()
        onward(way, i)
        if crosses(way, i):
            @pl.when(c == 1)
            def _():
                start_last(way, LAST.index((a, 0)))
                push(shard, piece).start()

            @pl.when(c == 0)
            def _():
                across(place(shard, piece), a, cross_recv.at[way, a]).start()
        else:
            push(shard, piece).start()

    for i in range(STEPS + LAG):
        if i == ANSWER:
            pl.when(c * PLANE + col == PLANE)(answer_all)
        if i == PASS:
            pl.when((col > 0) & (c == 1))(pass_on)
        for way in range(2):
            if i < STEPS:
                arrived(way, i)
            if i >= LAG and crosses(way, i - LAG):
                pl.when(c == 1)(functools.partial(from_partner, way, i - LAG))

    @pl.when(c == 1)
    def _():
        for t, (a, other) in enumerate(LAST):
            for way in range(2):
                def take(cross):
                    last(way, t, 4, cross).wait_recv()
                    push(shard_of(way, 4, lax.rem(c + other, CORES)), (a, *cross[way])).start()

                by_target(way, 4, take)

    @pl.when(c == 1)
    def _():
        message(partner, every, every).wait_send()
        over_chip(total_v, total_v).wait_send()

    @pl.when((col > 0) & (c == 1))
    def _():
        to_root().wait_send()
        answer(partner).wait_send()

    @pl.when(c * PLANE + col == PLANE)
    def _():
        ref = ins.at[0, pl.ds(0, 16 * PLANE)]
        pltpu.make_async_remote_copy(
            src_ref=ref, dst_ref=ref, send_sem=answer_send, recv_sem=answer_recv,
            device_id=partner, device_id_type=MESH,
        ).wait_send()

    @pl.when(c == 0)
    def _():
        over_chip(msg, both).wait_send()
        answer(partner).wait_recv()

    norm[...] = norm_f32[...].astype(jnp.bfloat16)

    def sent_early(rows):
        ref = ins.at[pl.ds(0, rows // HALF), pl.ds(0, HALF)]
        hop(0, 0, ref, ref, early_send).wait_send()

    def sent_ring(a, rows):
        ref = rows_of(a, rows)
        hop(0, 0, ref, ref, ici_send.at[a]).wait_send()

    def finish(core):
        def _():
            early_rows = EARLY_AT[core][-1]
            if core == 0:
                pl.when(z == 1)(functools.partial(sent_early, 2 * early_rows + ROWS))
                pl.when(z != 1)(functools.partial(sent_early, 2 * early_rows))
            else:
                sent_early(2 * early_rows)
            for a in range(3):
                own = sum(n for b, _, n in FIRST[core][EARLY[core] :] if b == a)
                ring_rows = 2 * (own + 2 * ROWS + (ROWS if core else 0))
                fewer = 2 * (SPLIT - LESS)
                pushed = ROWS + 2 * (3 * ROWS + (ROWS if core else 0))
                crossing = sum(p[2] for way in (0, 1) for i, (_, p) in enumerate(BASE[way]) if crosses(way, i) and p[0] == a)
                come = ROWS + 2 * 3 * ROWS + (-crossing if core else 2 * ROWS)
                ref = rows_of(a, come)
                across(ref, a, push_recv.at[a]).wait_recv()
                if core == 1:
                    pl.when(z == Z - 1)(functools.partial(sent_ring, a, ring_rows - fewer))
                    pl.when(z == 1)(functools.partial(sent_ring, a, ring_rows + fewer))
                    pl.when((z > 1) & (z < Z - 1) | (z == 0))(functools.partial(sent_ring, a, ring_rows))
                elif a == 1:
                    pl.when(z == 1)(functools.partial(sent_ring, a, ring_rows - ROWS))
                    pl.when(z != 1)(functools.partial(sent_ring, a, ring_rows))
                else:
                    sent_ring(a, ring_rows)
                ref = rows_of(a, pushed)
                across(ref, a, push_recv.at[a]).wait_send()

        return _

    for core in range(CORES):
        pl.when(c == core)(finish(core))


def store_kernel(*refs):
    ins, outs, sem = refs[:7], refs[7:14], refs[14]
    for i, (src, dst) in enumerate(zip(ins, outs)):
        parts = PARTS if i < 3 else 1
        rows = src.shape[0] // parts
        for p in range(parts):
            window = pl.ds(p * rows, rows)
            pltpu.make_async_copy(src.at[window], dst.at[window], sem.at[i]).start()
    for i, (src, dst) in enumerate(zip(ins, outs)):
        pltpu.make_async_copy(src, dst, sem.at[i]).wait()


def store(arrays):
    return pl.pallas_call(
        store_kernel,
        name="store",
        out_shape=tuple(jax.ShapeDtypeStruct(a.shape, a.dtype) for a in arrays),
        in_specs=[pl.BlockSpec(memory_space=pltpu.VMEM)] * 7,
        out_specs=(pl.BlockSpec(memory_space=pltpu.HBM),) * 7,
        scratch_shapes=[pltpu.SemaphoreType.DMA((7,))],
        compiler_params=pltpu.CompilerParams(vmem_limit_bytes=16 * 2**20),
    )(*arrays)


def per_device(oq, tq, ok, tk, ov, tv, share, train, step):
    f32, bf16 = jnp.float32, jnp.bfloat16
    whole = jax.ShapeDtypeStruct((SHARDS * ROWS, 2 * LANES), bf16)
    scale = jax.ShapeDtypeStruct((1, 2 * LANES), f32)
    vmem = pl.BlockSpec(memory_space=pltpu.VMEM)
    dma = pltpu.SemaphoreType.DMA
    outs = pl.pallas_call(
        kernel,
        name="mix_and_gather",
        out_shape=(whole, whole, whole, scale, scale, scale, jax.ShapeDtypeStruct((32, LANES), bf16)),
        in_specs=[pl.BlockSpec(memory_space=pltpu.HBM)] * 9,
        out_specs=(vmem,) * 7,
        scratch_shapes=[
            pltpu.VMEM((6, ROWS, 2 * LANES), f32),
            pltpu.VMEM((1, ROWS), f32),
            pltpu.VMEM((2, 1, PIECE), f32),
            pltpu.VMEM((3, ROWS, 2 * LANES), f32),
            pltpu.VMEM((2, EARLY_ROWS + ROWS, 2 * LANES), f32),
            pltpu.VMEM((8, LANES), f32),
            pltpu.VMEM((8, LANES), f32),
            pltpu.VMEM((8, LANES), f32),
            pltpu.VMEM((Z, 8, LANES), f32),
            pltpu.VMEM((SHARDS, LANES), f32),
            pltpu.VMEM((PLANE, SHARDS, LANES), f32),
            pltpu.VMEM((32, LANES), f32),
            dma((5,)),
            dma,
            dma,
            dma,
            dma,
            dma,
            dma,
            dma,
            dma,
            dma,
            dma((3,)),
            dma((2, STEPS)),
            dma((3,)),
            dma((3,)),
            dma((2, 3)),
        ],
        compiler_params=pltpu.CompilerParams(
            collective_id=0, has_side_effects=True, vmem_limit_bytes=24 * 2**20
        ),
    )(*(pltpu.with_memory_space_constraint(a, pltpu.HBM) for a in (
        oq, tq, ok, tk, ov, tv, share.reshape(1, -1), train.reshape(1, -1), step.reshape(1, -1)
    )))
    q, k, v, scale_q, scale_k, scale_v, norm = store(outs)
    return q, k, v, scale_q.reshape(-1), scale_k.reshape(-1), scale_v.reshape(-1), norm.reshape(-1)


def solution(mesh):
    split = Mesh(mesh.devices.reshape(Z, CORES, PLANE_Y, PLANE_X), FSDP_COLS)
    block = P(FSDP, COLS)
    return jax.shard_map(
        per_device,
        mesh=split,
        in_specs=(block,) * 6 + (P(FSDP), P(FSDP_COLS), P(FSDP_COLS)),
        out_specs=(P(None, COLS),) * 3 + (P(COLS),) * 3 + (P(),),
        check_vma=False,
    )
```
